256 devices in a mesh: outer: 2 (over z_hi), dp: 8 (over z_lo, core), tensor: 16 (over x, y).
Axes of the slice: x: 4, y: 4, z: 8 (z_hi: 2, z_lo: 4; z = z_hi * 4 + z_lo), core: 2. Of those that a mesh axis runs over, the one named last changes fastest.
Arguments:
- attn: bfloat16 [4096, 8192], P(('outer', 'dp'), 'tensor'), may hold values from -6 to 6
- out_weight: bfloat16 [8192, 8192], P(None, 'tensor'), may hold values from -0.0625 to 0.0625
- resid: bfloat16 [4096, 8192], P(('outer', 'dp'), 'tensor'), may hold values from -8 to 8
- norm_gain: bfloat16 [8192], P('tensor'), may hold values from 0.5 to 1.5
- head: bfloat16 [8192], P('tensor'), may hold values from -1 to 1
- lengths: int32 [64], P(('outer', 'dp')), may hold values from 1 to 64
- pairs: int32 [64, 2], P(('outer', 'dp')), may hold values from 0 to 3, as said below
- pair_valid: int32 [64], P(('outer', 'dp')), may hold values from 0 to 1, as said below
- loss_scale: float32 [1], replicated, may hold values from 1024 to 8192
Outputs:
- loss: float32 [1], replicated
- grad_out_proj: float32 [8192, 8192], P(('outer', 'dp'), 'tensor')
- grad_gain: float32 [8192], P('tensor')
- grad_head: float32 [8192], P('tensor')
The draws below stay inside these ranges and needn't reach their ends.
Inputs may be any that keep to these rules, and one draw needn't show every extreme that they name: `pairs`: in each pair the two numbers differ; the first pair of each replica is valid. `pair_valid`: the first of each replica's 4 entries is 1.
All inputs are finite; a program needn't handle non-finite values.
Results may differ from the reference program's by a relative error of at most 0.003.
Values may be sent and summed in bfloat16 or wider, within the bound.
A program may use at most 128 MiB of HBM per device.

```python
import math
import jax
import jax.numpy as jnp
from jax import lax

D = 8192
SEQ_LEN = 64
SEQS_DEV = 4
PAIRS_DEV = 4
HD = 8192
SEQS = 64
TOKENS = 4096
PAIRS = 64


def head_vector(key):
    values = jax.random.normal(jax.random.fold_in(key, 41), (D,), jnp.float32) * (D // 16) ** (-0.5)
    return jnp.clip(values, -1.0, 1.0)


def draw_head(key, part):
    return head_vector(key).astype(jnp.bfloat16)


def draw_pairs(key, part):
    first = jax.random.randint(jax.random.fold_in(key, 11), (PAIRS,), 0, SEQS_DEV)
    step = jax.random.randint(jax.random.fold_in(key, 12), (PAIRS,), 1, SEQS_DEV)
    second = (first + step) % SEQS_DEV
    return jnp.stack([first, second], axis=1).astype(jnp.int32)


def draw_pair_valid(key, part):
    coin = jax.random.randint(jax.random.fold_in(key, 21), (PAIRS,), 0, 4)
    leading = jnp.arange(PAIRS) % PAIRS_DEV == 0
    return jnp.where(leading | (coin > 0), 1, 0).astype(jnp.int32)


def draw_resid(key, part):
    headv = head_vector(key)
    unit = headv * D ** 0.5 / jnp.sqrt(jnp.sum(headv * headv))
    rising = 0.5 * jnp.exp(jnp.log(4.0) * jnp.arange(D, dtype=jnp.float32) / D)
    rough = jax.random.uniform(jax.random.fold_in(key, 31), (D,), jnp.float32, 0.7, 1.4)
    shape = rising * rough
    base_var = jnp.mean(shape * shape)
    base = jax.random.normal(jax.random.fold_in(key, 34), (TOKENS, D), jnp.float32)
    rest = base * shape[None, :]
    spread = (base_var + 1.0) * jnp.ones((TOKENS, 1), jnp.float32)
    share = 0.3
    along = share / (1.0 - share * share) ** 0.5 * jnp.sqrt(spread)
    values = rest + along * unit[None, :]
    return jnp.clip(values, -8.0, 8.0).astype(jnp.bfloat16)


def plant(values, rng, least, high):
    longest = values.shape.index(max(values.shape))
    spots = []
    for shift in (0, 1):
        where = [jax.random.randint(jax.random.fold_in(rng, axis), (), 0, length) for axis, length in enumerate(values.shape)]
        where[longest] = (where[longest] + shift) % values.shape[longest]
        spots.append(tuple(where))
    return values.at[spots[0]].set(least).at[spots[1]].set(high)


def levels(rng, extent, shards, least, top_value):
    level, own = 1.0, jax.random.fold_in(rng, 6)
    for dim, parts in shards:
        steps = jnp.exp(jax.random.uniform(jax.random.fold_in(own, dim), (parts,), jnp.float32, least / len(shards), top_value / len(shards)))
        level = level * jnp.repeat(steps, extent[dim] // parts).reshape([-1 if axis == dim else 1 for axis in range(len(extent))])
    return level


def noise(own_key, extent, width, limit, split=(), kind=jnp.bfloat16):
    values = jax.random.normal(own_key, extent, jnp.float32) * width
    if len(split) > 0:
        values = levels(own_key, extent, split, -0.22, 0.18) * values
    return jnp.clip(values, min=-limit, max=limit).astype(kind)


def setup_inputs(seed: int = 0) -> dict:
    keys = jax.random.split(jax.random.key(seed), 10)
    attn = noise(keys[0], (TOKENS, HD), 1.0, 6.0, ((0, 16), (1, 16)))
    out_weight = noise(keys[1], (D, HD), HD ** -0.5, 0.0625, ((1, 16),))
    resid = draw_resid(jax.random.fold_in(keys[9], 71), 0)
    norm_gain = jnp.clip(1.0 + 0.1 * jax.random.normal(keys[3], (D,), jnp.float32), 0.5, 1.5).astype(jnp.bfloat16)
    head = draw_head(jax.random.fold_in(keys[9], 71), 0)
    lengths = plant(jax.random.randint(keys[5], (SEQS,), 1, SEQ_LEN + 1), jax.random.fold_in(keys[5], 1), 1, SEQ_LEN).astype(jnp.int32)
    pairs = draw_pairs(jax.random.fold_in(keys[9], 71), 0)
    pair_valid = draw_pair_valid(jax.random.fold_in(keys[9], 71), 0)
    loss_scale = jnp.clip(jnp.exp(jax.random.uniform(keys[8], (1,), jnp.float32, math.log(1024.0), math.log(8192.0))), 1024.0, 8192.0)
    return {"attn": attn, "out_weight": out_weight, "resid": resid, "norm_gain": norm_gain, "head": head, "lengths": lengths, "pairs": pairs, "pair_valid": pair_valid, "loss_scale": loss_scale}


def reference(attn, out_weight, resid, norm_gain, head, lengths, pairs, pair_valid, loss_scale):
    f32 = jnp.float32
    attn_f = attn.astype(f32)
    proj = jnp.dot(attn_f, out_weight.astype(f32).T)
    z = resid.astype(f32) + proj
    gain = norm_gain.astype(f32)
    headv = head.astype(f32)
    inv = 1.0 / jnp.sqrt(lax.optimization_barrier(jnp.mean(z * z, axis=1, keepdims=True)) + 1e-05)
    normed = z * inv * gain
    score = lax.optimization_barrier(jnp.sum(normed * headv, axis=1))
    live = (jnp.arange(SEQ_LEN)[None, :] < lengths[:, None]).astype(f32)
    lens = lengths.astype(f32)
    reward = lax.optimization_barrier(jnp.sum(score.reshape(SEQS, SEQ_LEN) * live, axis=1)) / lens
    offset = (jnp.arange(PAIRS) // PAIRS_DEV * SEQS_DEV).astype(jnp.int32)
    chosen = pairs[:, 0] + offset
    rejected = pairs[:, 1] + offset
    valid = pair_valid.astype(f32)
    margin = reward[chosen] - reward[rejected]
    count = jnp.sum(valid)
    loss = jnp.sum(valid * jax.nn.softplus(-margin)) / count
    dmargin = -loss_scale[0] * valid * jax.nn.sigmoid(-margin) / count
    dreward = jnp.zeros((SEQS,), f32).at[chosen].add(dmargin).at[rejected].add(-dmargin)
    dscore = ((dreward / lens)[:, None] * live).reshape(TOKENS)
    grad_head = lax.optimization_barrier(jnp.sum(dscore[:, None] * normed, axis=0))
    grad_gain = lax.optimization_barrier(jnp.sum(dscore[:, None] * headv * z * inv, axis=0))
    a = dscore[:, None] * headv * gain
    dproj = inv * a - z * inv ** 3 * lax.optimization_barrier(jnp.sum(a * z, axis=1, keepdims=True)) / D
    dproj = dproj.astype(jnp.bfloat16)
    grad_out_proj = jnp.dot(dproj.astype(f32).T, attn_f)
    return (loss.reshape(1), grad_out_proj, grad_gain, grad_head)
```

```python
import jax
import jax.numpy as jnp
from jax import lax
from jax.sharding import PartitionSpec as P

REP = ("outer", "dp")


def shards(attn, out_weight, resid, norm_gain, head, lengths, pairs, pair_valid, loss_scale):
    f32 = jnp.float32
    bf16 = jnp.bfloat16
    reps = 16
    cols = 16
    tok = attn.shape[0]
    part = tok // cols
    hd = attn.shape[1]
    feats = out_weight.shape[0] // reps
    width = out_weight.shape[0]
    seqs = lengths.shape[0]
    seq_len = tok // seqs
    r = lax.axis_index(REP)
    t = lax.axis_index("tensor")
    attn_all = lax.all_gather(attn, REP, axis=0, tiled=True)
    vec = jnp.stack([norm_gain, head])
    vec_all = lax.all_gather(vec, "tensor", axis=1, tiled=True)
    vec_r = lax.dynamic_slice(vec_all, (0, r * feats), (2, feats)).astype(f32)
    gain, headv = vec_r[0], vec_r[1]
    small = jnp.concatenate([lengths, pairs[:, 0], pairs[:, 1], pair_valid])
    small = lax.all_gather(small, REP, axis=0)
    lens_all, first, second, valid = (small[:, i * seqs : (i + 1) * seqs] for i in range(4))
    res = lax.all_to_all(resid, "tensor", split_axis=0, concat_axis=0, tiled=True)
    res = lax.all_to_all(res, REP, split_axis=0, concat_axis=0, tiled=True)
    w = lax.dynamic_slice(out_weight, (r * feats, 0), (feats, hd))
    part_sum = lax.dot_general(attn_all, w, (((1,), (1,)), ((), ())), preferred_element_type=f32)
    part_sum = part_sum.astype(bf16).reshape(reps, cols, part, feats).transpose(1, 0, 2, 3)
    part_sum = part_sum.reshape(cols * reps * part, feats)
    proj = lax.psum_scatter(part_sum, "tensor", scatter_dimension=0, tiled=True)
    z = res.astype(f32) + proj.astype(f32)
    stats = jnp.stack([jnp.sum(z * z, axis=1), jnp.sum(z * (gain * headv)[None, :], axis=1)])
    stats = lax.psum(stats, REP)
    inv = 1.0 / jnp.sqrt(stats[0] / width + 1e-05)
    score = inv * stats[1]
    per_seq = seq_len // part
    slot = (t % per_seq) * part + jnp.arange(part)
    seq = t // per_seq
    lens_mine = lens_all[:, seq]
    live = (slot[None, :] < lens_mine[:, None]).astype(f32)
    pool = jnp.sum(score.reshape(reps, part) * live, axis=1)
    onehot = (jnp.arange(seqs) == seq).astype(f32)
    rewards = lax.psum(pool[:, None] * onehot[None, :], "tensor") / lens_all.astype(f32)
    choose = jnp.arange(seqs)[None, None, :]
    select = (first[:, :, None] == choose).astype(f32) - (second[:, :, None] == choose).astype(f32)
    margin = jnp.sum(select * rewards[:, None, :], axis=2)
    vf = valid.astype(f32)
    count = jnp.sum(vf)
    loss = (jnp.sum(vf * jax.nn.softplus(-margin)) / count).reshape(1)
    dmargin = -loss_scale[0] * vf * jax.nn.sigmoid(-margin) / count
    dreward = jnp.sum(dmargin[:, :, None] * select, axis=1) / lens_all.astype(f32)
    dmine = dreward[:, seq]
    dscore = (live * dmine[:, None]).reshape(-1)
    k = inv * dscore
    c = inv * inv * dscore * score / width
    g = jnp.sum(k[:, None] * z, axis=0)
    dproj = (k[:, None] * (gain * headv)[None, :] - z * c[:, None]).astype(bf16)
    d_all = lax.all_gather(dproj, "tensor", axis=0, tiled=False)
    d_all = d_all.reshape(cols, reps, part, feats).transpose(1, 0, 2, 3).reshape(reps * tok, feats)
    out = lax.dot_general(d_all, attn_all, (((0,), (0,)), ((), ())), preferred_element_type=f32)
    g = lax.psum(g, "tensor")
    g = lax.all_gather(g, REP, axis=0)
    g = lax.dynamic_slice(g, (t, 0), (1, feats))[0]
    return (loss, out, g * head.astype(f32), g * norm_gain.astype(f32))


def solution(mesh):
    placed = (
        P(REP, "tensor"),
        P(None, "tensor"),
        P(REP, "tensor"),
        P("tensor"),
        P("tensor"),
        P(REP),
        P(REP, None),
        P(REP),
        P(),
    )
    return jax.shard_map(
        shards,
        mesh=mesh,
        in_specs=placed,
        out_specs=(P(), P(REP, "tensor"), P("tensor"), P("tensor")),
        check_vma=False,
    )
```

```python
import jax
import jax.numpy as jnp
from jax import lax
from jax.experimental import pallas as pl
from jax.experimental.pallas import tpu as pltpu
from jax.sharding import Mesh
from jax.sharding import PartitionSpec as P

F32 = jnp.float32
BF16 = jnp.bfloat16
MESH = pl.DeviceIdType.MESH
WIDTH = 8192
HIGH = lax.Precision.HIGHEST


def wrap(value, size):
    return lax.rem(value + size, size)


def body(scale, attn_hbm, w_hbm, resid_hbm, vec, small, loss_ref, out_ref, gg_ref, gh_ref,
         att, wbuf, resbuf, res, vecr, smr, pf, m1s, m2s, m3s, m1r, m2r, m3r, s1f,
         n1s, n2s, n3s, n1r, n2r, n3r, zf, zt, za, hgc, stat, sa, sb, ks, cs, kc, gmine, gr, dt,
         loc_sem, att_txz, att_txc, att_rx, att_half, res_tx, res_rx, vec_sem, sm_tx, sm_rx,
         rs_tx, rs_rx, ag_tx, ag_rx, sa_tx, sa_rx, sb_tx, sb_rx, g_tx, g_rx):
    zc, core, x, y = (lax.axis_index(n) for n in ("z", "c", "x", "y"))
    r = zc * 2 + core
    t = x * 4 + y
    other = 1 - core
    zp, zm = wrap(zc + 1, 8), wrap(zc - 1, 8)
    diag = r == t

    def rep_dev(rr, tt):
        return {"z": rr // 2, "c": lax.rem(rr, 2), "x": tt // 4, "y": lax.rem(tt, 4)}

    def send(src, dst, tx, rx, dev):
        pltpu.make_async_remote_copy(src_ref=src, dst_ref=dst, send_sem=tx, recv_sem=rx,
                                     device_id=dev, device_id_type=MESH).start()

    def await_(ref, sem):
        pltpu.make_async_copy(ref, ref, sem).wait()

    load_a = pltpu.make_async_copy(attn_hbm, att.at[0, core], loc_sem.at[0])
    load_w = pltpu.make_async_copy(w_hbm.at[pl.ds(pl.multiple_of(r * 512, 512), 512)], wbuf, loc_sem.at[1])
    load_r = pltpu.make_async_copy(resid_hbm, resbuf, loc_sem.at[2])
    load_a.start()
    load_r.start()
    load_w.start()

    barrier = pltpu.get_barrier_semaphore()

    def greet(j, carry):
        pl.semaphore_signal(barrier, 1, device_id=rep_dev(wrap(r + j, 16), t), device_id_type=MESH)
        pl.semaphore_signal(barrier, 1, device_id=rep_dev(r, wrap(t + j, 16)), device_id_type=MESH)
        return carry

    lax.fori_loop(1, 16, greet, 0)

    def greet2(j, carry):
        @pl.when(jnp.logical_not(diag & (j == t)))
        def _():
            pl.semaphore_signal(barrier, 1, device_id=rep_dev(t, j), device_id_type=MESH)

        @pl.when(jnp.logical_not(diag & (j == r)))
        def _():
            pl.semaphore_signal(barrier, 1, device_id=rep_dev(j, r), device_id_type=MESH)

        return carry

    lax.fori_loop(0, 16, greet2, 0)
    pl.semaphore_wait(barrier, jnp.where(diag, 60, 62))

    load_a.wait()
    send(att.at[0, core], att.at[2, core], att_txz, att_rx.at[2, core], {"z": zp})
    send(att.at[0, core], att.at[1, core], att_txz, att_rx.at[1, core], {"z": zm})
    send(att.at[0, core], att.at[0, core], att_txc, att_rx.at[0, core], {"c": other})

    smr[r] = small[...]

    def send_small(j, carry):
        send(smr.at[r], smr.at[r], sm_tx, sm_rx, rep_dev(wrap(r + j, 16), t))
        return carry

    lax.fori_loop(1, 16, send_small, 0)

    @pl.when(diag)
    def _():
        vecr[...] = vec[...]

    @pl.when(jnp.logical_not(diag))
    def _():
        send(vec, vecr, vec_sem.at[0], vec_sem.at[1], rep_dev(t, r))

    load_r.wait()

    def send_res(j, carry):
        rows = pl.ds(pl.multiple_of(j * 16, 16), 16)
        own = diag & (j == t)

        @pl.when(own)
        def _():
            res[r] = resbuf[rows, :]

        @pl.when(jnp.logical_not(own))
        def _():
            send(resbuf.at[rows, :], res.at[r], res_tx, res_rx, rep_dev(t, j))

        return carry

    lax.fori_loop(0, 16, send_res, 0)
    load_w.wait()

    @pl.when(jnp.logical_not(diag))
    def _():
        await_(vecr, vec_sem.at[1])

    for q in range(4):
        row = vecr[q : q + 1, :] * vecr[4 + q : 5 + q, :]
        hgc[q] = jnp.broadcast_to(row, (128, 128)).T

    quarters = []
    for q in range(4):
        first = "x" if q < 2 else "y"
        second = "y" if q < 2 else "x"
        a0, b0 = (x, y) if q < 2 else (y, x)
        s = 1 if q % 2 == 0 else -1
        quarters.append(dict(
            q=q, a0=a0, b0=b0, lanes=slice(q * 128, (q + 1) * 128),
            af=wrap(a0 + 2, 4), an=wrap(a0 + s, 4), ao=wrap(a0 - s, 4),
            bf=wrap(b0 + 2, 4), bn=wrap(b0 + s, 4), bo=wrap(b0 - s, 4),
            dan={first: wrap(a0 + s, 4)}, dao={first: wrap(a0 - s, 4)},
            dbn={second: wrap(b0 + s, 4)}, dbo={second: wrap(b0 - s, 4)},
        ))

    def chunk(k, g, a):
        if g["q"] < 2:
            v = pf[k, :, pl.ds(a, 1), :, :, g["lanes"]]
        else:
            v = pf[k, :, :, pl.ds(a, 1), :, g["lanes"]]
        return v.reshape(2, 4, 16, 128)

    def tcol(g, a, b):
        return a * 4 + b if g["q"] < 2 else b * 4 + a

    def step_a(k):
        @pl.when((k == 1) | (k == 3))
        def _():
            await_(att.at[k, core], att_rx.at[k, core])
            send(att.at[k, core], att.at[k + 2, core], att_txz, att_rx.at[k + 2, core], {"z": zm})
            send(att.at[k, core], att.at[k, core], att_txc, att_rx.at[k, core], {"c": other})
            await_(att.at[k + 1, core], att_rx.at[k + 1, core])
            send(att.at[k + 1, core], att.at[k + 3, core], att_txz, att_rx.at[k + 3, core], {"z": zp})
            send(att.at[k + 1, core], att.at[k + 1, core], att_txc, att_rx.at[k + 1, core], {"c": other})

        @pl.when(k == 5)
        def _():
            lo, hi = pl.ds(0, 128), pl.ds(128, 128)
            await_(att.at[5, core], att_rx.at[5, core])
            send(att.at[5, core, hi], att.at[7, core, hi], att_txz, att_half, {"z": zm})
            send(att.at[5, core], att.at[5, core], att_txc, att_rx.at[5, core], {"c": other})
            await_(att.at[6, core], att_rx.at[6, core])
            send(att.at[6, core, lo], att.at[7, core, lo], att_txz, att_rx.at[7, core], {"z": zp})
            send(att.at[6, core], att.at[6, core], att_txc, att_rx.at[6, core], {"c": other})

        @pl.when(k == 7)
        def _():
            lo, hi = pl.ds(0, 128), pl.ds(128, 128)
            await_(att.at[7, core, lo], att_rx.at[7, core])
            await_(att.at[7, core, hi], att_half)
            send(att.at[7, core], att.at[7, core], att_txc, att_rx.at[7, core], {"c": other})

        await_(att.at[k, other], att_rx.at[k, other])
        rows = att[k].reshape(512, 512)
        prod = lax.dot_general(rows, wbuf[...], (((1,), (1,)), ((), ())), preferred_element_type=F32)
        pf[k] = prod.reshape(2, 4, 4, 16, 512)
        for g in quarters:
            q = g["q"]
            m1s[q, k] = chunk(k, g, g["af"]).astype(BF16)
            send(m1s.at[q, k], m1r.at[q, k], rs_tx.at[0, q], rs_rx.at[0, q, k], g["dan"])
        for g in quarters:
            q = g["q"]
            m3s[q, k] = chunk(k, g, g["ao"]).astype(BF16)
            send(m3s.at[q, k], m3r.at[q, k], rs_tx.at[1, q], rs_rx.at[1, q, k], g["dao"])

    def step_b(k):
        for g in quarters:
            q = g["q"]
            await_(m1r.at[q, k], rs_rx.at[0, q, k])
            m2s[q, k] = (chunk(k, g, g["an"]) + m1r[q, k].astype(F32)).astype(BF16)
            send(m2s.at[q, k], m2r.at[q, k], rs_tx.at[2, q], rs_rx.at[2, q, k], g["dan"])

    def step_c(k):
        for g in quarters:
            q = g["q"]
            await_(m3r.at[q, k], rs_rx.at[1, q, k])
            await_(m2r.at[q, k], rs_rx.at[2, q, k])
            s1f[q, k] = chunk(k, g, g["a0"]) + m2r[q, k].astype(F32) + m3r[q, k].astype(F32)
            n1s[q, k] = s1f[q, k, :, pl.ds(g["bf"], 1)].reshape(2, 16, 128).astype(BF16)
            send(n1s.at[q, k], n1r.at[q, k], rs_tx.at[3, q], rs_rx.at[3, q, k], g["dbn"])
            n3s[q, k] = s1f[q, k, :, pl.ds(g["bo"], 1)].reshape(2, 16, 128).astype(BF16)
            send(n3s.at[q, k], n3r.at[q, k], rs_tx.at[4, q], rs_rx.at[4, q, k], g["dbo"])

    def step_d(k):
        for g in quarters:
            q = g["q"]
            await_(n1r.at[q, k], rs_rx.at[3, q, k])
            n2s[q, k] = (s1f[q, k, :, pl.ds(g["bn"], 1)].reshape(2, 16, 128) + n1r[q, k].astype(F32)).astype(BF16)
            send(n2s.at[q, k], n2r.at[q, k], rs_tx.at[5, q], rs_rx.at[5, q, k], g["dbn"])

    def step_e(k):
        @pl.when(k == 0)
        def _():
            @pl.when(diag)
            def _():
                await_(res.at[pl.ds(0, 15)], res_rx)

            @pl.when(jnp.logical_not(diag))
            def _():
                await_(res, res_rx)

        off = ((k + 1) // 2) * (2 * lax.rem(k, 2) - 1)
        base = wrap(zc + off, 8) * 2
        for g in quarters:
            q = g["q"]
            await_(n2r.at[q, k], rs_rx.at[5, q, k])
            await_(n3r.at[q, k], rs_rx.at[4, q, k])
            total = s1f[q, k, :, pl.ds(g["b0"], 1)].reshape(2, 16, 128) + n2r[q, k].astype(F32) + n3r[q, k].astype(F32)
            zf[pl.ds(2 * k, 2), :, g["lanes"]] = total + res[pl.ds(base, 2), :, g["lanes"]].astype(F32)

    def flip(h):
        v = zf[8 * h : 8 * h + 8].reshape(128, 512)
        sq = jnp.zeros((1, 128), F32)
        dot = jnp.zeros((1, 128), F32)
        for q in range(4):
            turned = v[:, q * 128 : (q + 1) * 128].T
            zt[q, h] = turned
            za[h, t, q] = turned.astype(BF16)
            sq = sq + jnp.sum(turned * turned, axis=0, keepdims=True)
            dot = dot + jnp.sum(turned * hgc[q], axis=0, keepdims=True)
        stat[0:1, h * 128 : (h + 1) * 128] = sq
        stat[1:2, h * 128 : (h + 1) * 128] = dot

    def gsend(h, g, a, b, dev):
        q = g["q"]
        tt = tcol(g, a, b)
        send(za.at[h, tt, q], za.at[h, tt, q], ag_tx.at[q], ag_rx.at[h, q, tt], dev)

    def gwait(h, g, a, b):
        q = g["q"]
        tt = tcol(g, a, b)
        await_(za.at[h, tt, q], ag_rx.at[h, q, tt])

    def ag1(h):
        for g in quarters:
            gsend(h, g, g["a0"], g["b0"], g["dan"])
            gsend(h, g, g["a0"], g["b0"], g["dao"])
        for g in quarters:
            gsend(h, g, g["a0"], g["b0"], g["dbn"])
            gsend(h, g, g["a0"], g["b0"], g["dbo"])

    def ag2(h):
        for g in quarters:
            gwait(h, g, g["ao"], g["b0"])
            gsend(h, g, g["ao"], g["b0"], g["dan"])
        for g in quarters:
            gsend(h, g, g["ao"], g["b0"], g["dbn"])
            gsend(h, g, g["ao"], g["b0"], g["dbo"])
            gwait(h, g, g["an"], g["b0"])
            gsend(h, g, g["an"], g["b0"], g["dbn"])
            gsend(h, g, g["an"], g["b0"], g["dbo"])

    def ag3(h):
        for g in quarters:
            gwait(h, g, g["a0"], g["bo"])
            gsend(h, g, g["a0"], g["bo"], g["dbn"])
            gwait(h, g, g["af"], g["b0"])
            gsend(h, g, g["af"], g["b0"], g["dbn"])
            gsend(h, g, g["af"], g["b0"], g["dbo"])

    def ag4(h):
        for g in quarters:
            for a in ("ao", "an", "af"):
                gwait(h, g, g[a], g["bo"])
                gsend(h, g, g[a], g["bo"], g["dbn"])

    def ag5(h):
        for g in quarters:
            for a in ("a0", "ao", "an", "af"):
                gwait(h, g, g[a], g["bn"])
                gwait(h, g, g[a], g["bf"])

    def step(i, carry):
        @pl.when(i >= 4)
        def _():
            step_e(i - 4)

        @pl.when((i >= 3) & (i < 11))
        def _():
            step_d(i - 3)

        @pl.when((i >= 2) & (i < 10))
        def _():
            step_c(i - 2)

        @pl.when((i >= 1) & (i < 9))
        def _():
            step_b(i - 1)

        @pl.when(i < 8)
        def _():
            step_a(i)

        @pl.when(i == 7)
        def _():
            flip(0)
            ag1(0)

        @pl.when(i == 9)
        def _():
            ag2(0)

        @pl.when(i == 10)
        def _():
            ag3(0)

        @pl.when(i == 11)
        def _():
            ag4(0)

        return carry

    stat[...] = jnp.zeros((8, 256), F32)
    lax.fori_loop(0, 12, step, 0)
    flip(1)

    def absolute(lane):
        slot = lane >> 4
        k = slot >> 1
        off = ((k + 1) >> 1) * (2 * (k & 1) - 1)
        return ((((zc + off + 8) & 7) * 2 + (slot & 1)) << 4) + (lane & 15)

    rows256 = lax.broadcasted_iota(jnp.int32, (256, 256), 0)
    cols256 = lax.broadcasted_iota(jnp.int32, (256, 256), 1)
    to_abs = (absolute(rows256) == cols256).astype(F32)
    moved = jnp.dot(stat[...], to_abs, precision=HIGH, preferred_element_type=F32)
    sa[r] = jnp.zeros((8, 128), F32)
    sa[r, 0:1, :] = moved[0:1, 0:128]
    sa[r, 1:2, :] = moved[0:1, 128:256]
    sa[r, 2:3, :] = moved[1:2, 0:128]
    sa[r, 3:4, :] = moved[1:2, 128:256]

    def send_sa(j, carry):
        send(sa.at[r], sa.at[r], sa_tx, sa_rx, rep_dev(wrap(r + j, 16), t))
        return carry

    lax.fori_loop(1, 16, send_sa, 0)
    ag1(1)
    ag2(1)
    await_(sa.at[pl.ds(0, 15)], sa_rx)
    sb[t] = jnp.sum(sa[...], axis=0)

    def send_sb(j, carry):
        send(sb.at[t], sb.at[t], sb_tx, sb_rx, rep_dev(r, wrap(t + j, 16)))
        return carry

    lax.fori_loop(1, 16, send_sb, 0)
    ag3(1)
    await_(smr.at[pl.ds(0, 15)], sm_rx)
    await_(sb.at[pl.ds(0, 15)], sb_rx)

    ints = smr[:, 0, :].astype(F32)
    tsub = lax.broadcasted_iota(jnp.int32, (16, 128), 0)
    lane = lax.broadcasted_iota(jnp.int32, (16, 128), 1)
    group_r = lax.broadcasted_iota(jnp.int32, (16, 128), 0)
    bl_r = lax.broadcasted_iota(jnp.int32, (128, 128), 0)
    bl_c = lax.broadcasted_iota(jnp.int32, (128, 128), 1)
    block = ((bl_r >> 4) == (bl_c >> 4)).astype(F32)
    eight = lax.broadcasted_iota(jnp.int32, (8, 128), 0)
    halves = []
    count = jnp.zeros((1, 1), F32)
    loss_sum = jnp.zeros((1, 1), F32)
    for h in range(2):
        spread = ((lane >> 4) + 8 * h == group_r).astype(F32)
        ex = lax.dot_general(ints, spread, (((0,), (0,)), ((), ())), precision=HIGH, preferred_element_type=F32)
        lens = [ex[i : i + 1, :] for i in range(4)]
        firsts = [ex[4 + i : 5 + i, :] for i in range(4)]
        seconds = [ex[8 + i : 9 + i, :] for i in range(4)]
        valid = [ex[12 + i : 13 + i, :] for i in range(4)]
        inv = 1.0 / jnp.sqrt(sb[:, h, :] / WIDTH + 1e-05)
        score = inv * sb[:, 2 + h, :]
        lens16 = jnp.zeros((16, 128), F32)
        for i in range(4):
            lens16 = lens16 + jnp.where((tsub >> 2) == i, lens[i], 0.0)
        within = ((tsub & 3) * 16 + (lane & 15)).astype(F32)
        live = (within < lens16).astype(F32)
        pooled = score * live
        stack = jnp.zeros((8, 128), F32)
        for i in range(4):
            part = jnp.sum(jnp.where((tsub >> 2) == i, pooled, 0.0), axis=0, keepdims=True)
            stack = stack + jnp.where(eight == i, part, 0.0)
        summed = jnp.dot(stack, block, precision=HIGH, preferred_element_type=F32)
        reward = [summed[i : i + 1, :] / lens[i] for i in range(4)]
        weights = []
        for p in range(4):
            margin = jnp.zeros((1, 128), F32)
            for i in range(4):
                margin = margin + jnp.where(firsts[p] == i, reward[i], 0.0) - jnp.where(seconds[p] == i, reward[i], 0.0)
            soft = jnp.maximum(-margin, 0.0) + jnp.log1p(jnp.exp(-jnp.abs(margin)))
            loss_sum = loss_sum + jnp.sum(valid[p] * soft, axis=1, keepdims=True) * (1.0 / 16.0)
            count = count + jnp.sum(valid[p], axis=1, keepdims=True) * (1.0 / 16.0)
            weights.append(valid[p] / (1.0 + jnp.exp(margin)))
        halves.append((lens, firsts, seconds, inv, score, live, weights))
    loss_ref[...] = jnp.broadcast_to(loss_sum / count, (8, 128))
    factor = -scale[0] / count
    for h in range(2):
        lens, firsts, seconds, inv, score, live, weights = halves[h]
        dscore = jnp.zeros((16, 128), F32)
        for i in range(4):
            d = jnp.zeros((1, 128), F32)
            for p in range(4):
                w = weights[p] * factor
                d = d + jnp.where(firsts[p] == i, w, 0.0) - jnp.where(seconds[p] == i, w, 0.0)
            dscore = dscore + jnp.where((tsub >> 2) == i, d / lens[i], 0.0)
        dscore = dscore * live
        ks[:, h * 128 : (h + 1) * 128] = inv * dscore
        cs[:, h * 128 : (h + 1) * 128] = inv * inv * dscore * score * (1.0 / WIDTH)
    to_slot = (rows256 == absolute(cols256)).astype(F32)
    kslot = jnp.dot(ks[...], to_slot, precision=HIGH, preferred_element_type=F32)
    cslot = jnp.dot(cs[...], to_slot, precision=HIGH, preferred_element_type=F32)
    for i in range(16):
        kc[i, 0:1, :] = kslot[i : i + 1, :]
        kc[i, 1:2, :] = cslot[i : i + 1, :]

    krow = [kc[t, 0:1, 0:128], kc[t, 0:1, 128:256]]
    gsum = jnp.zeros((8, 128), F32)
    for q in range(4):
        prod = zt[q, 0] * krow[0] + zt[q, 1] * krow[1]
        row = jnp.sum(prod.T, axis=0, keepdims=True)
        gsum = gsum + jnp.where(eight == q, row, 0.0)
    gmine[...] = gsum

    def send_g(j, carry):
        own = diag & (j == r)

        @pl.when(own)
        def _():
            gr[t] = gmine[...]

        @pl.when(jnp.logical_not(own))
        def _():
            send(gmine, gr.at[t], g_tx, g_rx, rep_dev(j, r))

        return carry

    lax.fori_loop(0, 16, send_g, 0)
    ag4(1)

    def contract(h, first):
        def group(gi, carry):
            parts = []
            for j in range(4):
                tt = gi * 4 + j
                k1 = kc[tt, 0:1, h * 128 : (h + 1) * 128]
                c1 = kc[tt, 1:2, h * 128 : (h + 1) * 128]
                for q in range(4):
                    val = hgc[q] * k1 - za[h, tt, q].astype(F32) * c1
                    dt[q * 128 : (q + 1) * 128, j * 128 : (j + 1) * 128] = val.astype(BF16)
                parts.append(att[4 * h : 4 * h + 4, :, pl.ds(pl.multiple_of(tt * 16, 16), 16), :].reshape(128, 512))
            rhs = jnp.concatenate(parts, axis=0)
            prod = jnp.dot(dt[...], rhs, preferred_element_type=F32)

            if first:
                @pl.when(gi == 0)
                def _():
                    out_ref[...] = prod

                @pl.when(gi > 0)
                def _():
                    out_ref[...] += prod
            else:
                out_ref[...] += prod
            return carry

        lax.fori_loop(0, 4, group, 0)

    ag5(0)
    contract(0, True)
    ag5(1)
    contract(1, False)

    @pl.when(diag)
    def _():
        await_(gr.at[pl.ds(0, 15)], g_rx)
        await_(gr.at[pl.ds(0, 15)], g_tx)
        await_(res.at[pl.ds(0, 15)], res_tx)

    @pl.when(jnp.logical_not(diag))
    def _():
        await_(gr, g_rx)
        await_(gr, g_tx)
        await_(res, res_tx)
        await_(vecr, vec_sem.at[0])

    total = jnp.sum(gr[...], axis=0)
    gg_ref[...] = total[0:4, :] * vec[4:8, :]
    gh_ref[...] = total[0:4, :] * vec[0:4, :]

    await_(att.at[pl.ds(0, 7), 0], att_txz)
    await_(att.at[:, 0], att_txc)
    await_(smr.at[pl.ds(0, 15)], sm_tx)
    await_(sa.at[pl.ds(0, 15)], sa_tx)
    await_(sb.at[pl.ds(0, 15)], sb_tx)
    for q in range(4):
        for i, buf in enumerate((m1s, m3s, m2s, n1s, n3s, n2s)):
            await_(buf.at[q], rs_tx.at[i, q])
        await_(za.at[:, pl.ds(0, 15), q], ag_tx.at[q])


def shards(attn, out_weight, resid, norm_gain, head, lengths, pairs, pair_valid, loss_scale):
    vec = jnp.concatenate([norm_gain, head]).astype(F32).reshape(8, 128)
    small = jnp.concatenate([lengths, pairs[:, 0], pairs[:, 1], pair_valid])
    small = jnp.pad(small, (0, 1024 - small.shape[0])).reshape(8, 128)
    vm = pltpu.VMEM
    dma = pltpu.SemaphoreType.DMA
    big = (4, 8, 2, 4, 16, 128)
    little = (4, 8, 2, 16, 128)
    vspec = pl.BlockSpec(memory_space=pltpu.VMEM)
    anyspec = pl.BlockSpec(memory_space=pl.ANY)
    loss, out, gg, gh = pl.pallas_call(
        body,
        name="whole",
        out_shape=(
            jax.ShapeDtypeStruct((8, 128), F32),
            jax.ShapeDtypeStruct((512, 512), F32),
            jax.ShapeDtypeStruct((4, 128), F32),
            jax.ShapeDtypeStruct((4, 128), F32),
        ),
        in_specs=[pl.BlockSpec(memory_space=pltpu.SMEM), anyspec, anyspec, anyspec, vspec, vspec],
        out_specs=(vspec, vspec, vspec, vspec),
        scratch_shapes=[
            vm((8, 2, 256, 512), BF16), vm((512, 512), BF16), vm((256, 512), BF16), vm((16, 16, 512), BF16),
            vm((8, 128), F32), vm((16, 8, 128), jnp.int32), vm((8, 2, 4, 4, 16, 512), F32),
            vm(big, BF16), vm(big, BF16), vm(big, BF16), vm(big, BF16), vm(big, BF16), vm(big, BF16), vm(big, F32),
            vm(little, BF16), vm(little, BF16), vm(little, BF16), vm(little, BF16), vm(little, BF16), vm(little, BF16),
            vm((16, 16, 512), F32), vm((4, 2, 128, 128), F32), vm((2, 16, 4, 128, 128), BF16), vm((4, 128, 128), F32),
            vm((8, 256), F32), vm((16, 8, 128), F32), vm((16, 8, 128), F32), vm((16, 256), F32), vm((16, 256), F32), vm((16, 8, 256), F32),
            vm((8, 128), F32), vm((16, 8, 128), F32), vm((512, 512), BF16),
            dma((3,)), dma, dma, dma((8, 2)), dma, dma, dma, dma((2,)), dma, dma,
            dma((6, 4)), dma((6, 4, 8)), dma((4,)), dma((2, 4, 16)), dma, dma, dma, dma, dma, dma,
        ],
        compiler_params=pltpu.CompilerParams(collective_id=0, has_side_effects=True, vmem_limit_bytes=60 * 1024 * 1024),
    )(loss_scale, attn, out_weight, resid, vec, small)
    return (loss[0, 0:1], out, gg.reshape(512), gh.reshape(512))


def solution(mesh):
    finer = Mesh(mesh.devices.reshape(8, 2, 4, 4), ("z", "c", "x", "y"))
    rep, ten = ("z", "c"), ("x", "y")
    placed = (P(rep, ten), P(None, ten), P(rep, ten), P(ten), P(ten), P(rep), P(rep, None), P(rep), P())
    return jax.shard_map(
        shards,
        mesh=finer,
        in_specs=placed,
        out_specs=(P(), P(rep, ten), P(ten), P(ten)),
        check_vma=False,
    )
```

```python
import jax
import jax.numpy as jnp
from jax import lax
from jax.experimental import pallas as pl
from jax.experimental.pallas import tpu as pltpu
from jax.sharding import Mesh
from jax.sharding import PartitionSpec as P

F32 = jnp.float32
BF16 = jnp.bfloat16
MESH = pl.DeviceIdType.MESH
WIDTH = 8192
HIGH = lax.Precision.HIGHEST


def wrap(value, size):
    return lax.rem(value + size, size)


def body(scale, lens_ref, pairs_ref, valid_ref, attn_hbm, w_hbm, resid_hbm, gain_ref, head_ref, out_ref, misc_ref,
         att, wbuf, resbuf, rx, zo, zin, vec, vall, hgr, acc, smr, pf, m1s, m2s, m3s, m1r, m2r, m3r, s1f,
         n1s, n2s, n3s, n1r, n2r, n3r, zt, za, hgc, sa, sb, ks, cs, kc, gmine, gr, dt,
         loc_sem, w_sem, att_txz, att_txc, att_rx, att_rxc, r1_tx, r1_rx, zin_tx, zin_rx, vec_tx, vec_rx, sm_tx, sm_rx,
         rs_tx, rs_rx, ag_tx, ag_rx, sa_tx, sa_rx, sb_tx, sb_rx, g_tx, g_rx):
    zc, core, x, y = (lax.axis_index(n) for n in ("z", "c", "x", "y"))
    r = zc * 2 + core
    t = x * 4 + y
    other = 1 - core
    zp, zm = wrap(zc + 1, 8), wrap(zc - 1, 8)
    diag = r == t

    def rep_dev(rr, tt):
        return {"z": rr // 2, "c": lax.rem(rr, 2), "x": tt // 4, "y": lax.rem(tt, 4)}

    def send(src, dst, tx, rx, dev):
        pltpu.make_async_remote_copy(src_ref=src, dst_ref=dst, send_sem=tx, recv_sem=rx,
                                     device_id=dev, device_id_type=MESH).start()

    def await_(ref, sem):
        pltpu.make_async_copy(ref, ref, sem).wait()

    load_a = pltpu.make_async_copy(attn_hbm, att.at[0, core], loc_sem.at[0])
    load_r = pltpu.make_async_copy(resid_hbm, resbuf, loc_sem.at[1])
    load_a.start()

    def offset(k):
        return ((k + 1) // 2) * (2 * lax.rem(k, 2) - 1)

    def aim(k):
        return wrap(zc - offset(k), 8)

    def load_w(k, carry):
        rows = pl.ds(pl.multiple_of(aim(k) * 1024, 1024), 1024)
        pltpu.make_async_copy(w_hbm.at[rows], wbuf.at[k], w_sem.at[k]).start()
        return carry

    lax.fori_loop(0, 8, load_w, 0)
    load_r.start()

    barrier = pltpu.get_barrier_semaphore()

    def greet(j, carry):
        pl.semaphore_signal(barrier, 1, device_id=rep_dev(wrap(r + j, 16), t), device_id_type=MESH)
        pl.semaphore_signal(barrier, 1, device_id=rep_dev(r, wrap(t + j, 16)), device_id_type=MESH)
        return carry

    lax.fori_loop(1, 16, greet, 0)

    def greet2(j, carry):
        @pl.when(jnp.logical_not(diag & (j == t)))
        def _():
            pl.semaphore_signal(barrier, 1, device_id=rep_dev(t, j), device_id_type=MESH)

        @pl.when(jnp.logical_not(diag & (j == r)))
        def _():
            pl.semaphore_signal(barrier, 1, device_id=rep_dev(j, r), device_id_type=MESH)

        return carry

    lax.fori_loop(0, 16, greet2, 0)
    pl.semaphore_wait(barrier, jnp.where(diag, 60, 62))

    load_a.wait()
    def rows_of(j):
        return pl.ds(pl.multiple_of(j * 64, 64), 64)

    def up(k, j):
        return att.at[k, core, rows_of(lax.rem(j + 2, 4))]

    def down(k, j):
        return att.at[k, core, rows_of(j)]

    def send_own(j, carry):
        send(up(0, j), up(1, j), att_txz, att_rx.at[1, j], {"z": zm})
        send(down(0, j), down(2, j), att_txz, att_rx.at[2, j], {"z": zp})
        return carry

    lax.fori_loop(0, 4, send_own, 0)
    send(att.at[0, core], att.at[0, core], att_txc, att_rxc.at[0], {"c": other})

    def spread():
        lane8 = lax.broadcasted_iota(jnp.int32, (8, 128), 1)
        ints8 = jnp.zeros((8, 128), jnp.int32)
        for i in range(4):
            ints8 = jnp.where(lane8 == i, lens_ref[i], ints8)
            ints8 = jnp.where(lane8 == 4 + i, pairs_ref[0, i], ints8)
            ints8 = jnp.where(lane8 == 8 + i, pairs_ref[1, i], ints8)
            ints8 = jnp.where(lane8 == 12 + i, valid_ref[i], ints8)
        smr[r] = ints8
        vec[0:4, :] = gain_ref[...].astype(F32).reshape(4, 128)
        vec[4:8, :] = head_ref[...].astype(F32).reshape(4, 128)
        vall[t] = vec[...]
        load_r.wait()
        rx[t] = resbuf[pl.ds(pl.multiple_of(t * 16, 16), 16), :]
        acc[...] = jnp.zeros((2, 16, 128), F32)

        def one(j, carry):
            tt = wrap(t + j, 16)
            rows = pl.ds(pl.multiple_of(tt * 16, 16), 16)
            send(smr.at[r], smr.at[r], sm_tx, sm_rx, rep_dev(wrap(r + j, 16), t))
            send(vec, vall.at[t], vec_tx, vec_rx, rep_dev(r, tt))
            send(resbuf.at[rows, :], rx.at[t], r1_tx, r1_rx, rep_dev(r, tt))
            return carry

        lax.fori_loop(1, 16, one, 0)

    def gathered():
        await_(vall.at[pl.ds(0, 15)], vec_rx)
        await_(rx.at[pl.ds(0, 15)], r1_rx)
        hgr[...] = vall[:, 0:4, :] * vall[:, 4:8, :]
        for q in range(4):
            hgc[q] = jnp.broadcast_to(hgr[r, q : q + 1, :], (128, 128)).T

    quarters = []
    for q in range(4):
        first = "x" if q < 2 else "y"
        second = "y" if q < 2 else "x"
        a0, b0 = (x, y) if q < 2 else (y, x)
        s = 1 if q % 2 == 0 else -1
        quarters.append(dict(
            q=q, a0=a0, b0=b0, lanes=slice(q * 128, (q + 1) * 128),
            af=wrap(a0 + 2, 4), an=wrap(a0 + s, 4), ao=wrap(a0 - s, 4),
            bf=wrap(b0 + 2, 4), bn=wrap(b0 + s, 4), bo=wrap(b0 - s, 4),
            dan={first: wrap(a0 + s, 4)}, dao={first: wrap(a0 - s, 4)},
            dbn={second: wrap(b0 + s, 4)}, dbo={second: wrap(b0 - s, 4)},
        ))

    def chunk(k, g, a):
        if g["q"] < 2:
            v = pf[k, :, pl.ds(a, 1), :, :, g["lanes"]]
        else:
            v = pf[k, :, :, pl.ds(a, 1), :, g["lanes"]]
        return v.reshape(2, 4, 16, 128)

    def tcol(g, a, b):
        return a * 4 + b if g["q"] < 2 else b * 4 + a

    def ring(n):
        d, j = n // 4 + 1, lax.rem(n, 4)
        kp, km = 2 * d - 1, 2 * d

        @pl.when(n < 8)
        def _():
            await_(up(kp, j), att_rx.at[kp, j])
            send(up(kp, j), up(kp + 2, j), att_txz, att_rx.at[kp + 2, j], {"z": zm})
            await_(down(km, j), att_rx.at[km, j])
            send(down(km, j), down(km + 2, j), att_txz, att_rx.at[km + 2, j], {"z": zp})

        @pl.when((n >= 8) & (n < 12))
        def _():
            await_(up(5, j), att_rx.at[5, j])

            @pl.when(j < 2)
            def _():
                send(up(5, j), up(7, j), att_txz, att_rx.at[7, j], {"z": zm})

            await_(down(6, j), att_rx.at[6, j])

            @pl.when(j < 2)
            def _():
                send(down(6, j), down(7, j), att_txz, att_rx.at[7, j + 2], {"z": zp})

        @pl.when((j == 3) & (n < 12))
        def _():
            send(att.at[kp, core], att.at[kp, core], att_txc, att_rxc.at[kp], {"c": other})
            send(att.at[km, core], att.at[km, core], att_txc, att_rxc.at[km], {"c": other})

        @pl.when(n >= 12)
        def _():
            await_(up(7, j), att_rx.at[7, j])
            await_(down(7, j), att_rx.at[7, j + 2])

            @pl.when(j == 1)
            def _():
                send(att.at[7, core], att.at[7, core], att_txc, att_rxc.at[7], {"c": other})

    def step_a(k):
        await_(wbuf.at[k], w_sem.at[k])
        prod = lax.dot_general(att[0, core], wbuf[k], (((1,), (1,)), ((), ())), preferred_element_type=F32)
        pf[k, 0] = prod[:, 0:512].reshape(4, 4, 16, 512)
        pf[k, 1] = prod[:, 512:1024].reshape(4, 4, 16, 512)
        for g in quarters:
            q = g["q"]
            m1s[q, k] = chunk(k, g, g["af"]).astype(BF16)
            send(m1s.at[q, k], m1r.at[q, k], rs_tx.at[0, q], rs_rx.at[0, q, k], g["dan"])
        for g in quarters:
            q = g["q"]
            m3s[q, k] = chunk(k, g, g["ao"]).astype(BF16)
            send(m3s.at[q, k], m3r.at[q, k], rs_tx.at[1, q], rs_rx.at[1, q, k], g["dao"])

    def step_b(k):
        for g in quarters:
            q = g["q"]
            await_(m1r.at[q, k], rs_rx.at[0, q, k])
            m2s[q, k] = (chunk(k, g, g["an"]) + m1r[q, k].astype(F32)).astype(BF16)
            send(m2s.at[q, k], m2r.at[q, k], rs_tx.at[2, q], rs_rx.at[2, q, k], g["dan"])

    def step_c(k):
        for g in quarters:
            q = g["q"]
            await_(m3r.at[q, k], rs_rx.at[1, q, k])
            await_(m2r.at[q, k], rs_rx.at[2, q, k])
            s1f[q, k] = chunk(k, g, g["a0"]) + m2r[q, k].astype(F32) + m3r[q, k].astype(F32)
            n1s[q, k] = s1f[q, k, :, pl.ds(g["bf"], 1)].reshape(2, 16, 128).astype(BF16)
            send(n1s.at[q, k], n1r.at[q, k], rs_tx.at[3, q], rs_rx.at[3, q, k], g["dbn"])
            n3s[q, k] = s1f[q, k, :, pl.ds(g["bo"], 1)].reshape(2, 16, 128).astype(BF16)
            send(n3s.at[q, k], n3r.at[q, k], rs_tx.at[4, q], rs_rx.at[4, q, k], g["dbo"])

    def step_d(k):
        for g in quarters:
            q = g["q"]
            await_(n1r.at[q, k], rs_rx.at[3, q, k])
            n2s[q, k] = (s1f[q, k, :, pl.ds(g["bn"], 1)].reshape(2, 16, 128) + n1r[q, k].astype(F32)).astype(BF16)
            send(n2s.at[q, k], n2r.at[q, k], rs_tx.at[5, q], rs_rx.at[5, q, k], g["dbn"])

    def step_e(k):
        dz = aim(k)
        sq = jnp.zeros((16, 128), F32)
        dot = jnp.zeros((16, 128), F32)
        for g in quarters:
            q = g["q"]
            await_(n2r.at[q, k], rs_rx.at[5, q, k])
            await_(n3r.at[q, k], rs_rx.at[4, q, k])
            total = s1f[q, k, :, pl.ds(g["b0"], 1)].reshape(2, 16, 128) + n2r[q, k].astype(F32) + n3r[q, k].astype(F32)
            total = total + rx[pl.ds(2 * dz, 2), :, g["lanes"]].astype(F32)
            for cc in range(2):
                sq = sq + total[cc] * total[cc]
                dot = dot + total[cc] * hgr[2 * dz + cc, q : q + 1, :]
            zo[k, :, :, g["lanes"]] = total.astype(BF16)
        acc[0] += sq
        acc[1] += dot
        h = k // 4

        @pl.when(k == 0)
        def _():
            zin[core] = zo[0, core]

        @pl.when(k > 0)
        def _():
            send(zo.at[k, core], zin.at[2 * k + core], zin_tx.at[h], zin_rx.at[h], {"z": dz})

        send(zo.at[k, other], zin.at[2 * k + core], zin_tx.at[h], zin_rx.at[h], {"z": dz, "c": other})

    def flip(h):
        await_(zin.at[pl.ds(0, 7 + h)], zin_rx.at[h])
        v = zin[8 * h : 8 * h + 8].reshape(128, 512).astype(F32)
        for q in range(4):
            turned = v[:, q * 128 : (q + 1) * 128].T
            zt[q, h] = turned
            za[h, t, q] = turned.astype(BF16)

    def gsend(h, g, a, b, dev):
        q = g["q"]
        tt = tcol(g, a, b)
        send(za.at[h, tt, q], za.at[h, tt, q], ag_tx.at[q], ag_rx.at[h, q, tt], dev)

    def gwait(h, g, a, b):
        q = g["q"]
        tt = tcol(g, a, b)
        await_(za.at[h, tt, q], ag_rx.at[h, q, tt])

    def ag1(h):
        for g in quarters:
            gsend(h, g, g["a0"], g["b0"], g["dan"])
            gsend(h, g, g["a0"], g["b0"], g["dao"])
        for g in quarters:
            gsend(h, g, g["a0"], g["b0"], g["dbn"])
            gsend(h, g, g["a0"], g["b0"], g["dbo"])

    def ag2(h):
        for g in quarters:
            gwait(h, g, g["ao"], g["b0"])
            gsend(h, g, g["ao"], g["b0"], g["dan"])
        for g in quarters:
            gsend(h, g, g["ao"], g["b0"], g["dbn"])
            gsend(h, g, g["ao"], g["b0"], g["dbo"])
            gwait(h, g, g["an"], g["b0"])
            gsend(h, g, g["an"], g["b0"], g["dbn"])
            gsend(h, g, g["an"], g["b0"], g["dbo"])

    def ag3(h):
        for g in quarters:
            gwait(h, g, g["a0"], g["bo"])
            gsend(h, g, g["a0"], g["bo"], g["dbn"])
            gwait(h, g, g["af"], g["b0"])
            gsend(h, g, g["af"], g["b0"], g["dbn"])
            gsend(h, g, g["af"], g["b0"], g["dbo"])

    def ag4(h):
        for g in quarters:
            for a in ("ao", "an", "af"):
                gwait(h, g, g[a], g["bo"])
                gsend(h, g, g[a], g["bo"], g["dbn"])

    def ag5(h):
        for g in quarters:
            for a in ("a0", "ao", "an", "af"):
                gwait(h, g, g[a], g["bn"])
                gwait(h, g, g[a], g["bf"])

    def on(n, parity, first, fn):
        k = (n - first) // 2

        @pl.when((lax.rem(n, 2) == parity) & (n >= first) & (n < first + 16))
        def _():
            fn(k)

    def step(n, carry):
        @pl.when(n == 12)
        def _():
            gathered()

        on(n, 0, 12, step_e)
        on(n, 1, 9, step_d)
        on(n, 0, 6, step_c)
        on(n, 1, 3, step_b)
        on(n, 0, 0, step_a)

        @pl.when(n == 1)
        def _():
            spread()

        @pl.when((n >= 7) & (n < 21))
        def _():
            ring(n - 7)

        @pl.when(n == 21)
        def _():
            flip(0)
            ag1(0)

        @pl.when(n == 24)
        def _():
            ag2(0)

        @pl.when(n == 25)
        def _():
            ag3(0)

        return carry

    lax.fori_loop(0, 27, step, 0)

    def absolute(lane):
        slot = lane >> 4
        k = slot >> 1
        off = ((k + 1) >> 1) * (2 * (k & 1) - 1)
        return ((((zc + off + 8) & 7) * 2 + (slot & 1)) << 4) + (lane & 15)

    rows256 = lax.broadcasted_iota(jnp.int32, (256, 256), 0)
    cols256 = lax.broadcasted_iota(jnp.int32, (256, 256), 1)
    lane16 = lax.broadcasted_iota(jnp.int32, (16, 128), 1)
    row16 = lax.broadcasted_iota(jnp.int32, (16, 128), 0)
    pick = (lane16 & 15) == row16
    sa[r] = jnp.zeros((8, 128), F32)
    for i in range(2):
        column = jnp.sum(acc[i], axis=1, keepdims=True)
        sa[r, i : i + 1, :] = jnp.sum(jnp.where(pick, column, 0.0), axis=0, keepdims=True)

    def send_sa(j, carry):
        send(sa.at[r], sa.at[r], sa_tx, sa_rx, rep_dev(wrap(r + j, 16), t))
        return carry

    lax.fori_loop(1, 16, send_sa, 0)
    ag4(0)
    await_(sa.at[pl.ds(0, 15)], sa_rx)
    sb[t] = jnp.zeros((8, 128), F32)
    for i in range(2):
        for h in range(2):
            line = jnp.zeros((1, 128), F32)
            for j in range(8):
                line = line + jnp.where((lane16[0:1, :] >> 4) == j, sa[8 * h + j, i : i + 1, :], 0.0)
            sb[t, 2 * i + h : 2 * i + h + 1, :] = line

    def send_sb(j, carry):
        send(sb.at[t], sb.at[t], sb_tx, sb_rx, rep_dev(r, wrap(t + j, 16)))
        return carry

    lax.fori_loop(1, 16, send_sb, 0)
    flip(1)
    ag1(1)
    ag2(1)
    ag3(1)
    await_(smr.at[pl.ds(0, 15)], sm_rx)
    await_(sb.at[pl.ds(0, 15)], sb_rx)

    ints = smr[:, 0, :].astype(F32)
    tsub = lax.broadcasted_iota(jnp.int32, (16, 128), 0)
    lane = lax.broadcasted_iota(jnp.int32, (16, 128), 1)
    group_r = lax.broadcasted_iota(jnp.int32, (16, 128), 0)
    bl_r = lax.broadcasted_iota(jnp.int32, (128, 128), 0)
    bl_c = lax.broadcasted_iota(jnp.int32, (128, 128), 1)
    block = ((bl_r >> 4) == (bl_c >> 4)).astype(F32)
    eight = lax.broadcasted_iota(jnp.int32, (8, 128), 0)
    halves = []
    count = jnp.zeros((1, 1), F32)
    loss_sum = jnp.zeros((1, 1), F32)
    for h in range(2):
        spread = ((lane >> 4) + 8 * h == group_r).astype(F32)
        ex = lax.dot_general(ints, spread, (((0,), (0,)), ((), ())), precision=HIGH, preferred_element_type=F32)
        lens = [ex[i : i + 1, :] for i in range(4)]
        firsts = [ex[4 + i : 5 + i, :] for i in range(4)]
        seconds = [ex[8 + i : 9 + i, :] for i in range(4)]
        valid = [ex[12 + i : 13 + i, :] for i in range(4)]
        inv = 1.0 / jnp.sqrt(sb[:, h, :] / WIDTH + 1e-05)
        score = inv * sb[:, 2 + h, :]
        lens16 = jnp.zeros((16, 128), F32)
        for i in range(4):
            lens16 = lens16 + jnp.where((tsub >> 2) == i, lens[i], 0.0)
        within = ((tsub & 3) * 16 + (lane & 15)).astype(F32)
        live = (within < lens16).astype(F32)
        pooled = score * live
        stack = jnp.zeros((8, 128), F32)
        for i in range(4):
            part = jnp.sum(jnp.where((tsub >> 2) == i, pooled, 0.0), axis=0, keepdims=True)
            stack = stack + jnp.where(eight == i, part, 0.0)
        summed = jnp.dot(stack, block, precision=HIGH, preferred_element_type=F32)
        reward = [summed[i : i + 1, :] / lens[i] for i in range(4)]
        weights = []
        for p in range(4):
            margin = jnp.zeros((1, 128), F32)
            for i in range(4):
                margin = margin + jnp.where(firsts[p] == i, reward[i], 0.0) - jnp.where(seconds[p] == i, reward[i], 0.0)
            soft = jnp.maximum(-margin, 0.0) + jnp.log1p(jnp.exp(-jnp.abs(margin)))
            loss_sum = loss_sum + jnp.sum(valid[p] * soft, axis=1, keepdims=True) * (1.0 / 16.0)
            count = count + jnp.sum(valid[p], axis=1, keepdims=True) * (1.0 / 16.0)
            weights.append(valid[p] / (1.0 + jnp.exp(margin)))
        halves.append((lens, firsts, seconds, inv, score, live, weights))
    misc_ref[4:8, :] = jnp.broadcast_to(loss_sum / count, (4, 128))
    factor = -scale[0] / count
    for h in range(2):
        lens, firsts, seconds, inv, score, live, weights = halves[h]
        dscore = jnp.zeros((16, 128), F32)
        for i in range(4):
            d = jnp.zeros((1, 128), F32)
            for p in range(4):
                w = weights[p] * factor
                d = d + jnp.where(firsts[p] == i, w, 0.0) - jnp.where(seconds[p] == i, w, 0.0)
            dscore = dscore + jnp.where((tsub >> 2) == i, d / lens[i], 0.0)
        dscore = dscore * live
        ks[:, h * 128 : (h + 1) * 128] = inv * dscore
        cs[:, h * 128 : (h + 1) * 128] = inv * inv * dscore * score * (1.0 / WIDTH)
    to_slot = (rows256 == absolute(cols256)).astype(F32)
    kslot = jnp.dot(ks[...], to_slot, precision=HIGH, preferred_element_type=F32)
    cslot = jnp.dot(cs[...], to_slot, precision=HIGH, preferred_element_type=F32)
    for i in range(16):
        kc[i, 0:1, :] = kslot[i : i + 1, :]
        kc[i, 1:2, :] = cslot[i : i + 1, :]

    krow = [kc[t, 0:1, 0:128], kc[t, 0:1, 128:256]]
    gsum = jnp.zeros((8, 128), F32)
    for q in range(4):
        prod = zt[q, 0] * krow[0] + zt[q, 1] * krow[1]
        row = jnp.sum(prod.T, axis=0, keepdims=True)
        gsum = gsum + jnp.where(eight == q, row, 0.0)
    gmine[...] = gsum

    def send_g(j, carry):
        own = diag & (j == r)

        @pl.when(own)
        def _():
            gr[t] = gmine[...]

        @pl.when(jnp.logical_not(own))
        def _():
            send(gmine, gr.at[t], g_tx, g_rx, rep_dev(j, r))

        return carry

    lax.fori_loop(0, 16, send_g, 0)
    ag4(1)

    def contract(h, first):
        def group(gi, carry):
            parts = []
            for j in range(4):
                tt = gi * 4 + j
                k1 = kc[tt, 0:1, h * 128 : (h + 1) * 128]
                c1 = kc[tt, 1:2, h * 128 : (h + 1) * 128]
                for q in range(4):
                    val = hgc[q] * k1 - za[h, tt, q].astype(F32) * c1
                    dt[q * 128 : (q + 1) * 128, j * 128 : (j + 1) * 128] = val.astype(BF16)
                parts.append(att[4 * h : 4 * h + 4, :, pl.ds(pl.multiple_of(tt * 16, 16), 16), :].reshape(128, 512))
            rhs = jnp.concatenate(parts, axis=0)
            prod = jnp.dot(dt[...], rhs, preferred_element_type=F32)

            if first:
                @pl.when(gi == 0)
                def _():
                    out_ref[...] = prod

                @pl.when(gi > 0)
                def _():
                    out_ref[...] += prod
            else:
                out_ref[...] += prod
            return carry

        lax.fori_loop(0, 4, group, 0)

    for k in range(8):
        await_(att.at[k, other], att_rxc.at[k])
    ag5(0)
    contract(0, True)
    ag5(1)
    contract(1, False)

    @pl.when(diag)
    def _():
        await_(gr.at[pl.ds(0, 15)], g_rx)
        await_(gr.at[pl.ds(0, 15)], g_tx)

    @pl.when(jnp.logical_not(diag))
    def _():
        await_(gr, g_rx)
        await_(gr, g_tx)

    misc_ref[0:4, :] = jnp.sum(gr[...], axis=0)[0:4, :]

    await_(rx.at[pl.ds(0, 15)], r1_tx)
    await_(vall.at[pl.ds(0, 15)], vec_tx)
    await_(zin.at[pl.ds(0, 7)], zin_tx.at[0])
    await_(zin.at[pl.ds(0, 8)], zin_tx.at[1])
    await_(att.at[pl.ds(0, 7), 0], att_txz)
    await_(att.at[:, 0], att_txc)
    await_(smr.at[pl.ds(0, 15)], sm_tx)
    await_(sa.at[pl.ds(0, 15)], sa_tx)
    await_(sb.at[pl.ds(0, 15)], sb_tx)
    for q in range(4):
        for i, buf in enumerate((m1s, m3s, m2s, n1s, n3s, n2s)):
            await_(buf.at[q], rs_tx.at[i, q])
        await_(za.at[:, pl.ds(0, 15), q], ag_tx.at[q])


def shards(attn, out_weight, resid, norm_gain, head, lengths, pairs, pair_valid, loss_scale):
    vm = pltpu.VMEM
    dma = pltpu.SemaphoreType.DMA
    big = (4, 8, 2, 4, 16, 128)
    little = (4, 8, 2, 16, 128)
    vspec = pl.BlockSpec(memory_space=pltpu.VMEM)
    anyspec = pl.BlockSpec(memory_space=pl.ANY)
    smem = pl.BlockSpec(memory_space=pltpu.SMEM)
    out, misc = pl.pallas_call(
        body,
        name="whole",
        out_shape=(jax.ShapeDtypeStruct((512, 512), F32), jax.ShapeDtypeStruct((8, 128), F32)),
        in_specs=[smem, smem, smem, smem, anyspec, anyspec, anyspec, vspec, vspec],
        out_specs=(vspec, vspec),
        scratch_shapes=[
            vm((8, 2, 256, 512), BF16), vm((8, 1024, 512), BF16), vm((256, 512), BF16), vm((16, 16, 512), BF16),
            vm((8, 2, 16, 512), BF16), vm((16, 16, 512), BF16), vm((8, 128), F32), vm((16, 8, 128), F32), vm((16, 4, 128), F32),
            vm((2, 16, 128), F32), vm((16, 8, 128), jnp.int32), vm((8, 2, 4, 4, 16, 512), F32),
            vm(big, BF16), vm(big, BF16), vm(big, BF16), vm(big, BF16), vm(big, BF16), vm(big, BF16), vm(big, F32),
            vm(little, BF16), vm(little, BF16), vm(little, BF16), vm(little, BF16), vm(little, BF16), vm(little, BF16),
            vm((4, 2, 128, 128), F32), vm((2, 16, 4, 128, 128), BF16), vm((4, 128, 128), F32),
            vm((16, 8, 128), F32), vm((16, 8, 128), F32), vm((16, 256), F32), vm((16, 256), F32), vm((16, 8, 256), F32),
            vm((8, 128), F32), vm((16, 8, 128), F32), vm((512, 512), BF16),
            dma((2,)), dma((8,)), dma, dma, dma((8, 4)), dma((8,)), dma, dma, dma((2,)), dma((2,)), dma, dma, dma, dma,
            dma((6, 4)), dma((6, 4, 8)), dma((4,)), dma((2, 4, 16)), dma, dma, dma, dma, dma, dma,
        ],
        compiler_params=pltpu.CompilerParams(collective_id=0, has_side_effects=True, vmem_limit_bytes=60 * 1024 * 1024),
    )(loss_scale, lengths, pairs.T, pair_valid, attn, out_weight, resid, norm_gain, head)
    g = misc[0:4].reshape(512)
    return (misc[4, 0:1], out, g * head.astype(F32), g * norm_gain.astype(F32))


def solution(mesh):
    finer = Mesh(mesh.devices.reshape(8, 2, 4, 4), ("z", "c", "x", "y"))
    rep, ten = ("z", "c"), ("x", "y")
    placed = (P(rep, ten), P(None, ten), P(rep, ten), P(ten), P(ten), P(rep), P(rep, None), P(rep), P())
    return jax.shard_map(
        shards,
        mesh=finer,
        in_specs=placed,
        out_specs=(P(), P(rep, ten), P(ten), P(ten)),
        check_vma=False,
    )
```

```python
import jax
import jax.numpy as jnp
from jax import lax
from jax.experimental import pallas as pl
from jax.experimental.pallas import tpu as pltpu
from jax.sharding import Mesh
from jax.sharding import PartitionSpec as P

F32 = jnp.float32
BF16 = jnp.bfloat16
MESH = pl.DeviceIdType.MESH
WIDTH = 8192
HIGH = lax.Precision.HIGHEST


def wrap(value, size):
    return lax.rem(value + size, size)


def body(scale, lens_ref, pairs_ref, valid_ref, attn_hbm, w_hbm, resid_hbm, gain_ref, head_ref, out_ref, misc_ref,
         att, wbuf, resbuf, rx, zo, zin, zl, zlin, vec, vall, hgr, acc, smr, pf, m1s, m2s, m3s, m1r, m2r, m3r, s1f,
         n1s, n2s, n3s, n1r, n2r, n3r, za, hgc, sa, sb, ks, cs, kc, gmine, gr, dt,
         loc_sem, w_sem, att_txz, att_txc, att_rx, att_rxc, r1_tx, r1_rx, zin_tx, zin_rx, zl_tx, zl_rx, vec_tx, vec_rx, sm_tx, sm_rx,
         rs_tx, rs_rx, ag_tx, ag_rx, sa_tx, sa_rx, sb_tx, sb_rx, g_tx, g_rx):
    zc, core, x, y = (lax.axis_index(n) for n in ("z", "c", "x", "y"))
    r = zc * 2 + core
    t = x * 4 + y
    other = 1 - core
    zp, zm = wrap(zc + 1, 8), wrap(zc - 1, 8)
    diag = r == t

    def rep_dev(rr, tt):
        return {"z": rr // 2, "c": lax.rem(rr, 2), "x": tt // 4, "y": lax.rem(tt, 4)}

    def send(src, dst, tx, rx, dev):
        pltpu.make_async_remote_copy(src_ref=src, dst_ref=dst, send_sem=tx, recv_sem=rx,
                                     device_id=dev, device_id_type=MESH).start()

    def await_(ref, sem):
        pltpu.make_async_copy(ref, ref, sem).wait()

    load_a = pltpu.make_async_copy(attn_hbm, att.at[0, core], loc_sem.at[0])
    load_r = pltpu.make_async_copy(resid_hbm, resbuf, loc_sem.at[1])
    load_a.start()

    def place(k):
        return 7 - (4 * lax.rem(k // 2, 2) + 2 * (k // 4) + lax.rem(k, 2))

    def offset(k):
        m = place(k)
        return ((m + 1) // 2) * (2 * lax.rem(m, 2) - 1)

    def aim(k):
        return wrap(zc - offset(k), 8)

    def load_w(k, carry):
        rows = pl.ds(pl.multiple_of(aim(k) * 1024, 1024), 1024)
        pltpu.make_async_copy(w_hbm.at[rows], wbuf.at[k], w_sem.at[k]).start()
        return carry

    lax.fori_loop(0, 8, load_w, 0)
    load_r.start()

    barrier = pltpu.get_barrier_semaphore()

    def greet(j, carry):
        pl.semaphore_signal(barrier, 1, device_id=rep_dev(wrap(r + j, 16), t), device_id_type=MESH)
        pl.semaphore_signal(barrier, 1, device_id=rep_dev(r, wrap(t + j, 16)), device_id_type=MESH)
        return carry

    lax.fori_loop(1, 16, greet, 0)

    def greet2(j, carry):
        @pl.when(jnp.logical_not(diag & (j == t)))
        def _():
            pl.semaphore_signal(barrier, 1, device_id=rep_dev(t, j), device_id_type=MESH)

        @pl.when(jnp.logical_not(diag & (j == r)))
        def _():
            pl.semaphore_signal(barrier, 1, device_id=rep_dev(j, r), device_id_type=MESH)

        return carry

    lax.fori_loop(0, 16, greet2, 0)
    load_a.wait()

    def multiply(k):
        await_(wbuf.at[k], w_sem.at[k])
        prod = lax.dot_general(att[0, core], wbuf[k], (((1,), (1,)), ((), ())), preferred_element_type=F32)
        pf[k, 0] = prod[:, 0:512].reshape(4, 4, 16, 512)
        pf[k, 1] = prod[:, 512:1024].reshape(4, 4, 16, 512)

    multiply(0)
    pl.semaphore_wait(barrier, jnp.where(diag, 60, 62))

    def rows_of(j):
        return pl.ds(pl.multiple_of(j * 64, 64), 64)

    def up(k, j):
        return att.at[k, core, rows_of(lax.rem(j + 2, 4))]

    def down(k, j):
        return att.at[k, core, rows_of(j)]

    def send_own(j, carry):
        send(up(0, j), up(1, j), att_txz, att_rx.at[j], {"z": zm})
        send(down(0, j), down(2, j), att_txz, att_rx.at[j], {"z": zp})
        return carry

    lax.fori_loop(0, 4, send_own, 0)
    send(att.at[0, core], att.at[0, core], att_txc, att_rxc.at[1], {"c": other})

    def spread():
        lane8 = lax.broadcasted_iota(jnp.int32, (8, 128), 1)
        ints8 = jnp.zeros((8, 128), jnp.int32)
        for i in range(4):
            ints8 = jnp.where(lane8 == i, lens_ref[i], ints8)
            ints8 = jnp.where(lane8 == 4 + i, pairs_ref[0, i], ints8)
            ints8 = jnp.where(lane8 == 8 + i, pairs_ref[1, i], ints8)
            ints8 = jnp.where(lane8 == 12 + i, valid_ref[i], ints8)
        smr[r] = ints8
        vec[0:4, :] = gain_ref[...].astype(F32).reshape(4, 128)
        vec[4:8, :] = head_ref[...].astype(F32).reshape(4, 128)
        vall[t] = vec[...]
        load_r.wait()
        rx[t] = resbuf[pl.ds(pl.multiple_of(t * 16, 16), 16), :]
        acc[...] = jnp.zeros((2, 16, 128), F32)

    def pieces(n):
        def one(j, carry):
            tt = wrap(t + j, 16)
            rows = pl.ds(pl.multiple_of(tt * 16, 16), 16)
            send(smr.at[r], smr.at[r], sm_tx, sm_rx, rep_dev(wrap(r + j, 16), t))
            send(vec, vall.at[t], vec_tx, vec_rx, rep_dev(r, tt))
            send(resbuf.at[rows, :], rx.at[t], r1_tx, r1_rx, rep_dev(r, tt))
            return carry

        lax.fori_loop(3 * n - 2, 3 * n + 1, one, 0)

    def gathered():
        await_(vall.at[pl.ds(0, 15)], vec_rx)
        await_(rx.at[pl.ds(0, 15)], r1_rx)
        hgr[...] = vall[:, 0:4, :] * vall[:, 4:8, :]
        for q in range(4):
            hgc[q] = jnp.broadcast_to(hgr[r, q : q + 1, :], (128, 128)).T

    quarters = []
    for q in range(4):
        first = "x" if q < 2 else "y"
        second = "y" if q < 2 else "x"
        a0, b0 = (x, y) if q < 2 else (y, x)
        s = 1 if q % 2 == 0 else -1
        quarters.append(dict(
            q=q, a0=a0, b0=b0, lanes=slice(q * 128, (q + 1) * 128),
            af=wrap(a0 + 2, 4), an=wrap(a0 + s, 4), ao=wrap(a0 - s, 4),
            bf=wrap(b0 + 2, 4), bn=wrap(b0 + s, 4), bo=wrap(b0 - s, 4),
            dan={first: wrap(a0 + s, 4)}, dao={first: wrap(a0 - s, 4)},
            dbn={second: wrap(b0 + s, 4)}, dbo={second: wrap(b0 - s, 4)},
        ))

    def chunk(k, g, a):
        if g["q"] < 2:
            v = pf[k, :, pl.ds(a, 1), :, :, g["lanes"]]
        else:
            v = pf[k, :, :, pl.ds(a, 1), :, g["lanes"]]
        return v.reshape(2, 4, 16, 128)

    def tcol(g, a, b):
        return a * 4 + b if g["q"] < 2 else b * 4 + a

    def ring(n):
        n = jnp.int32(n)
        d, j = n // 4 + 1, lax.rem(n, 4)
        kp, km = 2 * d - 1, 2 * d
        await_(att.at[0, core, pl.ds(0, 128)], att_rx.at[n])

        @pl.when(n < 10)
        def _():
            send(up(kp, j), up(jnp.minimum(kp + 2, 7), j), att_txz, att_rx.at[n + 4], {"z": zm})
            send(down(km, j), down(jnp.minimum(km + 2, 7), j), att_txz, att_rx.at[n + 4], {"z": zp})

        @pl.when((j == 3) & (n < 12))
        def _():
            h = jnp.where((kp == 3) | (kp == 7), 0, 1)
            send(att.at[kp, core], att.at[kp, core], att_txc, att_rxc.at[h], {"c": other})
            h = jnp.where((km == 2) | (km == 6), 0, 1)
            send(att.at[km, core], att.at[km, core], att_txc, att_rxc.at[h], {"c": other})

        @pl.when(n == 13)
        def _():
            send(att.at[7, core], att.at[7, core], att_txc, att_rxc.at[0], {"c": other})

    def step_a(k):
        @pl.when(k > 0)
        def _():
            multiply(k)

        for g in quarters:
            q = g["q"]
            m1s[q, k] = chunk(k, g, g["af"]).astype(BF16)
            send(m1s.at[q, k], m1r.at[q, k], rs_tx.at[0], rs_rx.at[0, k], g["dan"])
        for g in quarters:
            q = g["q"]
            m3s[q, k] = chunk(k, g, g["ao"]).astype(BF16)
            send(m3s.at[q, k], m3r.at[q, k], rs_tx.at[1], rs_rx.at[1, k], g["dao"])

    def step_b(k):
        await_(m1r.at[:, k], rs_rx.at[0, k])
        for g in quarters:
            q = g["q"]
            m2s[q, k] = (chunk(k, g, g["an"]) + m1r[q, k].astype(F32)).astype(BF16)
            send(m2s.at[q, k], m2r.at[q, k], rs_tx.at[2], rs_rx.at[2, k], g["dan"])

    def step_c(k):
        await_(m3r.at[:, k], rs_rx.at[1, k])
        await_(m2r.at[:, k], rs_rx.at[2, k])
        for g in quarters:
            q = g["q"]
            s1f[q, k] = chunk(k, g, g["a0"]) + m2r[q, k].astype(F32) + m3r[q, k].astype(F32)
            n1s[q, k] = s1f[q, k, :, pl.ds(g["bf"], 1)].reshape(2, 16, 128).astype(BF16)
            send(n1s.at[q, k], n1r.at[q, k], rs_tx.at[3], rs_rx.at[3, k], g["dbn"])
            n3s[q, k] = s1f[q, k, :, pl.ds(g["bo"], 1)].reshape(2, 16, 128).astype(BF16)
            send(n3s.at[q, k], n3r.at[q, k], rs_tx.at[4], rs_rx.at[4, k], g["dbo"])

    def step_d(k):
        await_(n1r.at[:, k], rs_rx.at[3, k])
        for g in quarters:
            q = g["q"]
            n2s[q, k] = (s1f[q, k, :, pl.ds(g["bn"], 1)].reshape(2, 16, 128) + n1r[q, k].astype(F32)).astype(BF16)
            send(n2s.at[q, k], n2r.at[q, k], rs_tx.at[5], rs_rx.at[5, k], g["dbn"])

    def step_e(k):
        dz = aim(k)
        sq = jnp.zeros((16, 128), F32)
        dot = jnp.zeros((16, 128), F32)
        await_(n2r.at[:, k], rs_rx.at[5, k])
        await_(n3r.at[:, k], rs_rx.at[4, k])
        for g in quarters:
            q = g["q"]
            total = s1f[q, k, :, pl.ds(g["b0"], 1)].reshape(2, 16, 128) + n2r[q, k].astype(F32) + n3r[q, k].astype(F32)
            total = total + rx[pl.ds(2 * dz, 2), :, g["lanes"]].astype(F32)
            for cc in range(2):
                sq = sq + total[cc] * total[cc]
                dot = dot + total[cc] * hgr[2 * dz + cc, q : q + 1, :]
            high = total.astype(BF16)
            zo[k, :, :, g["lanes"]] = high
            zl[k, :, :, g["lanes"]] = (total - high.astype(F32)).astype(BF16)
        acc[0] += sq
        acc[1] += dot
        h = k // 4

        @pl.when(k == 7)
        def _():
            zin[14 + core] = zo[7, core]

        @pl.when(k < 7)
        def _():
            send(zo.at[k, core], zin.at[2 * k + core], zin_tx.at[h], zin_rx.at[h], {"z": dz})

        send(zo.at[k, other], zin.at[2 * k + core], zin_tx.at[h], zin_rx.at[h], {"z": dz, "c": other})

    def send_low(k, carry):
        dz = aim(k)

        @pl.when(k == 7)
        def _():
            zlin[14 + core] = zl[7, core]

        @pl.when(k < 7)
        def _():
            send(zl.at[k, core], zlin.at[2 * k + core], zl_tx, zl_rx, {"z": dz})

        send(zl.at[k, other], zlin.at[2 * k + core], zl_tx, zl_rx, {"z": dz, "c": other})
        return carry

    def flip(h):
        await_(zin.at[pl.ds(0, 8 - h)], zin_rx.at[h])
        v = zin[8 * h : 8 * h + 8].reshape(128, 512).astype(F32)
        for q in range(4):
            za[h, t, q] = v[:, q * 128 : (q + 1) * 128].T.astype(BF16)

    def gsend(h, g, a, b, dev, event):
        q = g["q"]
        tt = tcol(g, g[a], g[b])
        send(za.at[h, tt, q], za.at[h, tt, q], ag_tx, ag_rx.at[h, event], g[dev])

    def gwait(h, event):
        await_(za.at[h, 0], ag_rx.at[h, event])

    def ag1(h):
        for g in quarters:
            gsend(h, g, "a0", "b0", "dan", 0)
            gsend(h, g, "a0", "b0", "dao", 1)
        for g in quarters:
            gsend(h, g, "a0", "b0", "dbn", 3)
            gsend(h, g, "a0", "b0", "dbo", 7)

    def ag2(h):
        gwait(h, 0)
        for g in quarters:
            gsend(h, g, "ao", "b0", "dan", 2)
        for g in quarters:
            gsend(h, g, "ao", "b0", "dbn", 4)
        gwait(h, 1)
        for g in quarters:
            gsend(h, g, "an", "b0", "dbn", 5)
        for g in quarters:
            gsend(h, g, "ao", "b0", "dbo", 7)
            gsend(h, g, "an", "b0", "dbo", 7)

    def ag3(h):
        gwait(h, 3)
        for g in quarters:
            gsend(h, g, "a0", "bo", "dbn", 7)
        gwait(h, 2)
        for g in quarters:
            gsend(h, g, "af", "b0", "dbn", 6)
        for g in quarters:
            gsend(h, g, "af", "b0", "dbo", 7)

    def ag4part(h, i):
        gwait(h, 4 + i)
        for g in quarters:
            gsend(h, g, ("ao", "an", "af")[i], "bo", "dbn", 7)

    def ag4(h):
        for i in range(3):
            ag4part(h, i)

    def ag5(h):
        await_(za.at[h, pl.ds(0, 8)], ag_rx.at[h, 7])

    def on(n, parity, first, fn):
        k = (n - first) // 2

        @pl.when((lax.rem(n, 2) == parity) & (n >= first) & (n < first + 16))
        def _():
            fn(k)

    def step(n, carry):
        @pl.when(n == 12)
        def _():
            gathered()

        on(n, 0, 12, step_e)
        on(n, 1, 9, step_d)
        on(n, 0, 6, step_c)
        on(n, 1, 3, step_b)
        on(n, 0, 0, step_a)

        @pl.when(n == 0)
        def _():
            spread()

        @pl.when((n >= 1) & (n < 6))
        def _():
            pieces(n)

        @pl.when((n >= 5) & (lax.rem(n, 2) == 1))
        def _():
            ring((n - 5) // 2)

        @pl.when(n == 21)
        def _():
            flip(0)
            ag1(0)

        return carry

    lax.fori_loop(0, 27, step, 0)

    def absolute(lane):
        slot = lane >> 4
        k = slot >> 1
        m = 7 - (4 * ((k >> 1) & 1) + 2 * (k >> 2) + (k & 1))
        off = ((m + 1) >> 1) * (2 * (m & 1) - 1)
        return ((((zc + off + 8) & 7) * 2 + (slot & 1)) << 4) + (lane & 15)

    rows256 = lax.broadcasted_iota(jnp.int32, (256, 256), 0)
    cols256 = lax.broadcasted_iota(jnp.int32, (256, 256), 1)
    lane16 = lax.broadcasted_iota(jnp.int32, (16, 128), 1)
    row16 = lax.broadcasted_iota(jnp.int32, (16, 128), 0)
    pick = (lane16 & 15) == row16
    sa[r] = jnp.zeros((8, 128), F32)
    for i in range(2):
        column = jnp.sum(acc[i], axis=1, keepdims=True)
        sa[r, i : i + 1, :] = jnp.sum(jnp.where(pick, column, 0.0), axis=0, keepdims=True)

    def send_sa(j, carry):
        send(sa.at[r], sa.at[r], sa_tx, sa_rx, rep_dev(wrap(r + j, 16), t))
        return carry

    lax.fori_loop(1, 16, send_sa, 0)
    lax.fori_loop(0, 8, send_low, 0)
    ag2(0)
    flip(1)
    ag1(1)
    ag3(0)
    await_(sa.at[pl.ds(0, 15)], sa_rx)
    sb[t] = jnp.zeros((8, 128), F32)
    for i in range(2):
        for h in range(2):
            line = jnp.zeros((1, 128), F32)
            for j in range(8):
                line = line + jnp.where((lane16[0:1, :] >> 4) == j, sa[8 * h + j, i : i + 1, :], 0.0)
            sb[t, 2 * i + h : 2 * i + h + 1, :] = line

    def send_sb(j, carry):
        send(sb.at[t], sb.at[t], sb_tx, sb_rx, rep_dev(r, wrap(t + j, 16)))
        return carry

    lax.fori_loop(1, 16, send_sb, 0)
    ag2(1)
    ring(11)
    ag4(0)
    ring(12)
    ring(13)
    ag3(1)
    ag4part(1, 0)
    ag4part(1, 1)
    await_(smr.at[pl.ds(0, 15)], sm_rx)
    await_(sb.at[pl.ds(0, 15)], sb_rx)

    ints = smr[:, 0, :].astype(F32)
    tsub = lax.broadcasted_iota(jnp.int32, (16, 128), 0)
    lane = lax.broadcasted_iota(jnp.int32, (16, 128), 1)
    group_r = lax.broadcasted_iota(jnp.int32, (16, 128), 0)
    bl_r = lax.broadcasted_iota(jnp.int32, (128, 128), 0)
    bl_c = lax.broadcasted_iota(jnp.int32, (128, 128), 1)
    block = ((bl_r >> 4) == (bl_c >> 4)).astype(F32)
    eight = lax.broadcasted_iota(jnp.int32, (8, 128), 0)
    halves = []
    count = jnp.zeros((1, 1), F32)
    loss_sum = jnp.zeros((1, 1), F32)
    for h in range(2):
        spread = ((lane >> 4) + 8 * h == group_r).astype(F32)
        ex = lax.dot_general(ints, spread, (((0,), (0,)), ((), ())), precision=HIGH, preferred_element_type=F32)
        lens = [ex[i : i + 1, :] for i in range(4)]
        firsts = [ex[4 + i : 5 + i, :] for i in range(4)]
        seconds = [ex[8 + i : 9 + i, :] for i in range(4)]
        valid = [ex[12 + i : 13 + i, :] for i in range(4)]
        inv = 1.0 / jnp.sqrt(sb[:, h, :] / WIDTH + 1e-05)
        score = inv * sb[:, 2 + h, :]
        lens16 = jnp.zeros((16, 128), F32)
        for i in range(4):
            lens16 = lens16 + jnp.where((tsub >> 2) == i, lens[i], 0.0)
        within = ((tsub & 3) * 16 + (lane & 15)).astype(F32)
        live = (within < lens16).astype(F32)
        pooled = score * live
        stack = jnp.zeros((8, 128), F32)
        for i in range(4):
            part = jnp.sum(jnp.where((tsub >> 2) == i, pooled, 0.0), axis=0, keepdims=True)
            stack = stack + jnp.where(eight == i, part, 0.0)
        summed = jnp.dot(stack, block, precision=HIGH, preferred_element_type=F32)
        reward = [summed[i : i + 1, :] / lens[i] for i in range(4)]
        weights = []
        for p in range(4):
            margin = jnp.zeros((1, 128), F32)
            for i in range(4):
                margin = margin + jnp.where(firsts[p] == i, reward[i], 0.0) - jnp.where(seconds[p] == i, reward[i], 0.0)
            soft = jnp.maximum(-margin, 0.0) + jnp.log1p(jnp.exp(-jnp.abs(margin)))
            loss_sum = loss_sum + jnp.sum(valid[p] * soft, axis=1, keepdims=True) * (1.0 / 16.0)
            count = count + jnp.sum(valid[p], axis=1, keepdims=True) * (1.0 / 16.0)
            weights.append(valid[p] / (1.0 + jnp.exp(margin)))
        halves.append((lens, firsts, seconds, inv, score, live, weights))
    misc_ref[4:8, :] = jnp.broadcast_to(loss_sum / count, (4, 128))
    factor = -scale[0] / count
    for h in range(2):
        lens, firsts, seconds, inv, score, live, weights = halves[h]
        dscore = jnp.zeros((16, 128), F32)
        for i in range(4):
            d = jnp.zeros((1, 128), F32)
            for p in range(4):
                w = weights[p] * factor
                d = d + jnp.where(firsts[p] == i, w, 0.0) - jnp.where(seconds[p] == i, w, 0.0)
            dscore = dscore + jnp.where((tsub >> 2) == i, d / lens[i], 0.0)
        dscore = dscore * live
        ks[:, h * 128 : (h + 1) * 128] = inv * dscore
        cs[:, h * 128 : (h + 1) * 128] = inv * inv * dscore * score * (1.0 / WIDTH)
    to_slot = (rows256 == absolute(cols256)).astype(F32)
    kslot = jnp.dot(ks[...], to_slot, precision=HIGH, preferred_element_type=F32)
    cslot = jnp.dot(cs[...], to_slot, precision=HIGH, preferred_element_type=F32)
    for i in range(16):
        kc[i, 0:1, :] = kslot[i : i + 1, :]
        kc[i, 1:2, :] = cslot[i : i + 1, :]

    await_(zlin.at[pl.ds(0, 15)], zl_rx)
    krow = [kc[t, 0:1, 0:128], kc[t, 0:1, 128:256]]
    gsum = jnp.zeros((8, 128), F32)
    for q in range(4):
        row = jnp.zeros((1, 128), F32)
        for h in range(2):
            column = jnp.broadcast_to(krow[h], (128, 128)).T
            full = zin[8 * h : 8 * h + 8, :, q * 128 : (q + 1) * 128].astype(F32)
            full = full + zlin[8 * h : 8 * h + 8, :, q * 128 : (q + 1) * 128].astype(F32)
            row = row + jnp.sum(full.reshape(128, 128) * column, axis=0, keepdims=True)
        gsum = gsum + jnp.where(eight == q, row, 0.0)
    gmine[...] = gsum

    def send_g(j, carry):
        own = diag & (j == r)

        @pl.when(own)
        def _():
            gr[t] = gmine[...]

        @pl.when(jnp.logical_not(own))
        def _():
            send(gmine, gr.at[t], g_tx, g_rx, rep_dev(j, r))

        return carry

    lax.fori_loop(0, 16, send_g, 0)

    def contract(h, first):
        def group(gi, carry):
            if first:
                @pl.when(gi == 1)
                def _():
                    ag4part(1, 2)

            parts = []
            for j in range(4):
                tt = gi * 4 + j
                k1 = kc[tt, 0:1, h * 128 : (h + 1) * 128]
                c1 = kc[tt, 1:2, h * 128 : (h + 1) * 128]
                for q in range(4):
                    val = hgc[q] * k1 - za[h, tt, q].astype(F32) * c1
                    dt[q * 128 : (q + 1) * 128, j * 128 : (j + 1) * 128] = val.astype(BF16)
                rows = pl.ds(pl.multiple_of(tt * 16, 16), 16)
                for k in range(4 * h, 4 * h + 4):
                    parts.append(att[7 - (4 * (k // 2 % 2) + 2 * (k // 4) + k % 2), :, rows, :].reshape(32, 512))
            rhs = jnp.concatenate(parts, axis=0)
            prod = jnp.dot(dt[...], rhs, preferred_element_type=F32)

            if first:
                @pl.when(gi == 0)
                def _():
                    out_ref[...] = prod

                @pl.when(gi > 0)
                def _():
                    out_ref[...] += prod
            else:
                out_ref[...] += prod
            return carry

        lax.fori_loop(0, 4, group, 0)

    await_(att.at[pl.ds(0, 4), 0], att_rxc.at[0])
    await_(att.at[pl.ds(0, 4), 0], att_rxc.at[1])
    ag5(0)
    contract(0, True)
    ag5(1)
    contract(1, False)

    @pl.when(diag)
    def _():
        await_(gr.at[pl.ds(0, 15)], g_rx)
        await_(gr.at[pl.ds(0, 15)], g_tx)

    @pl.when(jnp.logical_not(diag))
    def _():
        await_(gr, g_rx)
        await_(gr, g_tx)

    misc_ref[0:4, :] = jnp.sum(gr[...], axis=0)[0:4, :]

    await_(rx.at[pl.ds(0, 15)], r1_tx)
    await_(vall.at[pl.ds(0, 15)], vec_tx)
    await_(zin.at[pl.ds(0, 8)], zin_tx.at[0])
    await_(zlin.at[pl.ds(0, 15)], zl_tx)
    await_(zin.at[pl.ds(0, 7)], zin_tx.at[1])
    await_(att.at[pl.ds(0, 7), 0], att_txz)
    await_(att.at[:, 0], att_txc)
    await_(smr.at[pl.ds(0, 15)], sm_tx)
    await_(sa.at[pl.ds(0, 15)], sa_tx)
    await_(sb.at[pl.ds(0, 15)], sb_tx)
    for i, buf in enumerate((m1s, m3s, m2s, n1s, n3s, n2s)):
        await_(buf, rs_tx.at[i])
    await_(za.at[:, pl.ds(0, 15)], ag_tx)


def shards(attn, out_weight, resid, norm_gain, head, lengths, pairs, pair_valid, loss_scale):
    vm = pltpu.VMEM
    dma = pltpu.SemaphoreType.DMA
    big = (4, 8, 2, 4, 16, 128)
    little = (4, 8, 2, 16, 128)
    vspec = pl.BlockSpec(memory_space=pltpu.VMEM)
    anyspec = pl.BlockSpec(memory_space=pltpu.HBM)
    smem = pl.BlockSpec(memory_space=pltpu.SMEM)
    out, misc = pl.pallas_call(
        body,
        name="whole",
        out_shape=(jax.ShapeDtypeStruct((512, 512), F32), jax.ShapeDtypeStruct((8, 128), F32)),
        in_specs=[smem, smem, smem, smem, anyspec, anyspec, anyspec, vspec, vspec],
        out_specs=(vspec, vspec),
        scratch_shapes=[
            vm((8, 2, 256, 512), BF16), vm((8, 1024, 512), BF16), vm((256, 512), BF16), vm((16, 16, 512), BF16),
            vm((8, 2, 16, 512), BF16), vm((16, 16, 512), BF16), vm((8, 2, 16, 512), BF16), vm((16, 16, 512), BF16), vm((8, 128), F32), vm((16, 8, 128), F32), vm((16, 4, 128), F32),
            vm((2, 16, 128), F32), vm((16, 8, 128), jnp.int32), vm((8, 2, 4, 4, 16, 512), F32),
            vm(big, BF16), vm(big, BF16), vm(big, BF16), vm(big, BF16), vm(big, BF16), vm(big, BF16), vm(big, F32),
            vm(little, BF16), vm(little, BF16), vm(little, BF16), vm(little, BF16), vm(little, BF16), vm(little, BF16),
            vm((2, 16, 4, 128, 128), BF16), vm((4, 128, 128), F32),
            vm((16, 8, 128), F32), vm((16, 8, 128), F32), vm((16, 256), F32), vm((16, 256), F32), vm((16, 8, 256), F32),
            vm((8, 128), F32), vm((16, 8, 128), F32), vm((512, 512), BF16),
            dma((2,)), dma((8,)), dma, dma, dma((14,)), dma((2,)), dma, dma, dma((2,)), dma((2,)), dma, dma, dma, dma, dma, dma,
            dma((6,)), dma((6, 8)), dma, dma((2, 8)), dma, dma, dma, dma, dma, dma,
        ],
        compiler_params=pltpu.CompilerParams(collective_id=0, has_side_effects=True, vmem_limit_bytes=60 * 1024 * 1024),
    )(loss_scale, lengths, pairs.T, pair_valid, attn, out_weight, resid, norm_gain, head)
    g = misc[0:4].reshape(512)
    return (misc[4, 0:1], out, g * head.astype(F32), g * norm_gain.astype(F32))


def solution(mesh):
    finer = Mesh(mesh.devices.reshape(8, 2, 4, 4), ("z", "c", "x", "y"))
    rep, ten = ("z", "c"), ("x", "y")
    placed = (P(rep, ten), P(None, ten), P(rep, ten), P(ten), P(ten), P(rep), P(rep, None), P(rep), P())
    return jax.shard_map(
        shards,
        mesh=finer,
        in_specs=placed,
        out_specs=(P(), P(rep, ten), P(ten), P(ten)),
        check_vma=False,
    )
```

```python
import jax
import jax.numpy as jnp
from jax import lax
from jax.experimental import pallas as pl
from jax.experimental.pallas import tpu as pltpu
from jax.sharding import Mesh
from jax.sharding import PartitionSpec as P

F32 = jnp.float32
BF16 = jnp.bfloat16
MESH = pl.DeviceIdType.MESH
WIDTH = 8192
HIGH = lax.Precision.HIGHEST


def wrap(value, size):
    return lax.rem(value + size, size)


def body(scale, lens_hbm, pairs_hbm, valid_hbm, attn_hbm, w_hbm, resid_hbm, gain_hbm, head_hbm, out_ref, misc_ref,
         lens_ref, pairs_ref, valid_ref, gain_ref, head_ref, att, wbuf, resbuf, rx, zo, zin, zl, zlin, vec, vall, hgr, acc, hl, vsum, dd, smr, pf, m1s, m2s, m3s, m1r, m2r, m3r, s1f,
         n1s, n2s, n3s, n1r, n2r, n3r, za, hgc, sa, sb, ks, cs, kc, gmine, gr, dt,
         loc_sem, small_sem, w_sem, att_txz, att_txc, att_rx, att_rxc, r1_tx, r1_rx, zin_tx, zin_rx, zl_tx, zl_rx, vec_tx, vec_rx, sm_tx, sm_rx,
         rs_tx, rs_rx, ag_tx, ag_rx, sa_tx, sa_rx, sb_tx, sb_rx, g_tx, g_rx, dd_tx, dd_rx):
    zc, core, x, y = (lax.axis_index(n) for n in ("z", "c", "x", "y"))
    r = zc * 2 + core
    t = x * 4 + y
    other = 1 - core
    zp, zm = wrap(zc + 1, 8), wrap(zc - 1, 8)
    diag = r == t

    def rep_dev(rr, tt):
        return {"z": rr // 2, "c": lax.rem(rr, 2), "x": tt // 4, "y": lax.rem(tt, 4)}

    def send(src, dst, tx, rx, dev):
        pltpu.make_async_remote_copy(src_ref=src, dst_ref=dst, send_sem=tx, recv_sem=rx,
                                     device_id=dev, device_id_type=MESH).start()

    def await_(ref, sem):
        pltpu.make_async_copy(ref, ref, sem).wait()

    load_a = pltpu.make_async_copy(attn_hbm, att.at[0, core], loc_sem.at[0])
    load_r = pltpu.make_async_copy(resid_hbm, resbuf, loc_sem.at[1])
    load_a.start()
    loads = [
        pltpu.make_async_copy(a, b, small_sem.at[i])
        for i, (a, b) in enumerate((
            (lens_hbm, lens_ref), (pairs_hbm, pairs_ref), (valid_hbm, valid_ref), (gain_hbm, gain_ref), (head_hbm, head_ref)
        ))
    ]

    def place(k):
        return 7 - (4 * lax.rem(k // 2, 2) + 2 * (k // 4) + lax.rem(k, 2))

    def offset(k):
        m = place(k)
        return ((m + 1) // 2) * (2 * lax.rem(m, 2) - 1)

    def aim(k):
        return wrap(zc - offset(k), 8)

    def load_w(k, carry):
        rows = pl.ds(pl.multiple_of(aim(k) * 1024, 1024), 1024)
        pltpu.make_async_copy(w_hbm.at[rows], wbuf.at[k], w_sem.at[k]).start()
        return carry

    load_w(0, 0)

    barrier = pltpu.get_barrier_semaphore()

    def greet(j, carry):
        pl.semaphore_signal(barrier, 1, device_id=rep_dev(wrap(r + j, 16), t), device_id_type=MESH)
        pl.semaphore_signal(barrier, 1, device_id=rep_dev(r, wrap(t + j, 16)), device_id_type=MESH)
        return carry

    lax.fori_loop(1, 16, greet, 0)

    def greet2(j, carry):
        @pl.when(jnp.logical_not(diag & (j == t)))
        def _():
            pl.semaphore_signal(barrier, 1, device_id=rep_dev(t, j), device_id_type=MESH)

        @pl.when(jnp.logical_not(diag & (j == r)))
        def _():
            pl.semaphore_signal(barrier, 1, device_id=rep_dev(j, r), device_id_type=MESH)

        return carry

    lax.fori_loop(0, 16, greet2, 0)
    lax.fori_loop(1, 8, load_w, 0)
    load_r.start()
    for load in loads:
        load.start()
    load_a.wait()

    def multiply(k):
        await_(wbuf.at[k], w_sem.at[k])
        prod = lax.dot_general(att[0, core], wbuf[k], (((1,), (1,)), ((), ())), preferred_element_type=F32)
        pf[k, 0] = prod[:, 0:512].reshape(4, 4, 16, 512)
        pf[k, 1] = prod[:, 512:1024].reshape(4, 4, 16, 512)

    multiply(0)
    pl.semaphore_wait(barrier, jnp.where(diag, 60, 62))

    def rows_of(j):
        return pl.ds(pl.multiple_of(j * 64, 64), 64)

    def up(k, j):
        return att.at[k, core, rows_of(lax.rem(j + 2, 4))]

    def down(k, j):
        return att.at[k, core, rows_of(j)]

    def send_own(j, carry):
        send(up(0, j), up(1, j), att_txz, att_rx.at[j], {"z": zm})
        send(down(0, j), down(2, j), att_txz, att_rx.at[j], {"z": zp})
        return carry

    lax.fori_loop(0, 4, send_own, 0)
    send(att.at[0, core], att.at[0, core], att_txc, att_rxc.at[1], {"c": other})

    def spread():
        for load in loads:
            load.wait()
        lane8 = lax.broadcasted_iota(jnp.int32, (8, 128), 1)
        ints8 = jnp.zeros((8, 128), jnp.int32)
        for i in range(4):
            ints8 = jnp.where(lane8 == i, lens_ref[i], ints8)
            ints8 = jnp.where(lane8 == 4 + i, pairs_ref[0, i], ints8)
            ints8 = jnp.where(lane8 == 8 + i, pairs_ref[1, i], ints8)
            ints8 = jnp.where(lane8 == 12 + i, valid_ref[i], ints8)
        smr[r] = ints8
        vec[0:4, :] = gain_ref[...].astype(F32).reshape(4, 128)
        vec[4:8, :] = head_ref[...].astype(F32).reshape(4, 128)
        vall[t] = vec[...]
        load_r.wait()
        rx[t] = resbuf[pl.ds(pl.multiple_of(t * 16, 16), 16), :]
        acc[...] = jnp.zeros((16, 128), F32)
        hl[...] = jnp.zeros((8, 1024), F32)
        vsum[...] = jnp.zeros((8, 512), F32)

    def pieces(n):
        def one(j, carry):
            tt = wrap(t + j, 16)
            rows = pl.ds(pl.multiple_of(tt * 16, 16), 16)
            send(smr.at[r], smr.at[r], sm_tx, sm_rx, rep_dev(wrap(r + j, 16), t))
            send(vec, vall.at[t], vec_tx, vec_rx, rep_dev(r, tt))
            send(resbuf.at[rows, :], rx.at[t], r1_tx, r1_rx, rep_dev(r, tt))
            return carry

        lax.fori_loop(3 * n - 2, 3 * n + 1, one, 0)

    def gathered():
        await_(vall.at[pl.ds(0, 15)], vec_rx)
        await_(rx.at[pl.ds(0, 15)], r1_rx)
        hgr[...] = vall[:, 0:4, :] * vall[:, 4:8, :]
        for q in range(4):
            hgc[q] = jnp.broadcast_to(hgr[r, q : q + 1, :], (128, 128)).T

    quarters = []
    for q in range(4):
        first = "x" if q < 2 else "y"
        second = "y" if q < 2 else "x"
        a0, b0 = (x, y) if q < 2 else (y, x)
        s = 1 if q % 2 == 0 else -1
        quarters.append(dict(
            q=q, a0=a0, b0=b0, lanes=slice(q * 128, (q + 1) * 128),
            af=wrap(a0 + 2, 4), an=wrap(a0 + s, 4), ao=wrap(a0 - s, 4),
            bf=wrap(b0 + 2, 4), bn=wrap(b0 + s, 4), bo=wrap(b0 - s, 4),
            dan={first: wrap(a0 + s, 4)}, dao={first: wrap(a0 - s, 4)},
            dbn={second: wrap(b0 + s, 4)}, dbo={second: wrap(b0 - s, 4)},
        ))

    def chunk(k, g, a):
        if g["q"] < 2:
            v = pf[k, :, pl.ds(a, 1), :, :, g["lanes"]]
        else:
            v = pf[k, :, :, pl.ds(a, 1), :, g["lanes"]]
        return v.reshape(2, 4, 16, 128)

    def tcol(g, a, b):
        return a * 4 + b if g["q"] < 2 else b * 4 + a

    def ring(n):
        n = jnp.int32(n)
        d, j = n // 4 + 1, lax.rem(n, 4)
        kp, km = 2 * d - 1, 2 * d
        await_(att.at[0, core, pl.ds(0, 128)], att_rx.at[n])

        @pl.when(n < 10)
        def _():
            send(up(kp, j), up(jnp.minimum(kp + 2, 7), j), att_txz, att_rx.at[n + 4], {"z": zm})
            send(down(km, j), down(jnp.minimum(km + 2, 7), j), att_txz, att_rx.at[n + 4], {"z": zp})

        @pl.when((j == 3) & (n < 12))
        def _():
            h = jnp.where((kp == 3) | (kp == 7), 0, 1)
            send(att.at[kp, core], att.at[kp, core], att_txc, att_rxc.at[h], {"c": other})
            h = jnp.where((km == 2) | (km == 6), 0, 1)
            send(att.at[km, core], att.at[km, core], att_txc, att_rxc.at[h], {"c": other})

        @pl.when(n == 13)
        def _():
            send(att.at[7, core], att.at[7, core], att_txc, att_rxc.at[0], {"c": other})

    def step_a(k):
        @pl.when(k > 0)
        def _():
            multiply(k)

        for g in quarters:
            q = g["q"]
            m1s[q, k] = chunk(k, g, g["af"]).astype(BF16)
            send(m1s.at[q, k], m1r.at[q, k], rs_tx.at[0], rs_rx.at[0, k], g["dan"])
        for g in quarters:
            q = g["q"]
            m3s[q, k] = chunk(k, g, g["ao"]).astype(BF16)
            send(m3s.at[q, k], m3r.at[q, k], rs_tx.at[1], rs_rx.at[1, k], g["dao"])

    def step_b(k):
        await_(m1r.at[:, k], rs_rx.at[0, k])
        for g in quarters:
            q = g["q"]
            m2s[q, k] = (chunk(k, g, g["an"]) + m1r[q, k].astype(F32)).astype(BF16)
            send(m2s.at[q, k], m2r.at[q, k], rs_tx.at[2], rs_rx.at[2, k], g["dan"])

    def step_c(k):
        await_(m3r.at[:, k], rs_rx.at[1, k])
        await_(m2r.at[:, k], rs_rx.at[2, k])
        for g in quarters:
            q = g["q"]
            s1f[q, k] = chunk(k, g, g["a0"]) + m2r[q, k].astype(F32) + m3r[q, k].astype(F32)
            n1s[q, k] = s1f[q, k, :, pl.ds(g["bf"], 1)].reshape(2, 16, 128).astype(BF16)
            send(n1s.at[q, k], n1r.at[q, k], rs_tx.at[3], rs_rx.at[3, k], g["dbn"])
            n3s[q, k] = s1f[q, k, :, pl.ds(g["bo"], 1)].reshape(2, 16, 128).astype(BF16)
            send(n3s.at[q, k], n3r.at[q, k], rs_tx.at[4], rs_rx.at[4, k], g["dbo"])

    def step_d(k):
        await_(n1r.at[:, k], rs_rx.at[3, k])
        for g in quarters:
            q = g["q"]
            n2s[q, k] = (s1f[q, k, :, pl.ds(g["bn"], 1)].reshape(2, 16, 128) + n1r[q, k].astype(F32)).astype(BF16)
            send(n2s.at[q, k], n2r.at[q, k], rs_tx.at[5], rs_rx.at[5, k], g["dbn"])

    def step_e(k):
        dz = aim(k)
        sq = jnp.zeros((16, 128), F32)
        await_(n2r.at[:, k], rs_rx.at[5, k])
        await_(n3r.at[:, k], rs_rx.at[4, k])
        for g in quarters:
            q = g["q"]
            total = s1f[q, k, :, pl.ds(g["b0"], 1)].reshape(2, 16, 128) + n2r[q, k].astype(F32) + n3r[q, k].astype(F32)
            total = total + rx[pl.ds(2 * dz, 2), :, g["lanes"]].astype(F32)
            for cc in range(2):
                sq = sq + total[cc] * total[cc]
            high = total.astype(BF16)
            zo[k, :, :, g["lanes"]] = high
            zl[k, :, :, g["lanes"]] = (total - high.astype(F32)).astype(BF16)
        acc[...] += sq
        h = k // 4

        @pl.when(k == 7)
        def _():
            zin[14 + core] = zo[7, core]

        @pl.when(k < 7)
        def _():
            send(zo.at[k, core], zin.at[2 * k + core], zin_tx.at[h], zin_rx.at[h], {"z": dz})

        send(zo.at[k, other], zin.at[2 * k + core], zin_tx.at[h], zin_rx.at[h], {"z": dz, "c": other})

    def halves_of(row):
        high = row.astype(BF16).astype(F32)
        return high, row - high

    def project_head(k):
        for cc in range(2):
            for q in range(4):
                at = slice((cc * 4 + q) * 128, (cc * 4 + q + 1) * 128)
                high, low = halves_of(hgr[2 * aim(k) + cc, q : q + 1, :])
                hl[0:1, at] = high
                hl[1:2, at] = low
        vsum[...] += jnp.dot(hl[...].astype(BF16), wbuf[k], preferred_element_type=F32)

    def head_dots():
        high, rest = halves_of(vsum[0:1, :] + vsum[1:2, :])
        middle, low = halves_of(rest)
        hl[0:1, 0:512] = high
        hl[1:2, 0:512] = middle
        hl[2:3, 0:512] = low
        for q in range(4):
            at = slice(512 + q * 128, 640 + q * 128)
            high, low = halves_of(hgr[t, q : q + 1, :])
            hl[0:1, at] = high
            hl[1:2, at] = low
        rows = hl[...].astype(BF16)
        along = (((1,), (1,)), ((), ()))
        a = lax.dot_general(rows[:, 0:512], att[0, core], along, preferred_element_type=F32)
        b = lax.dot_general(rows[:, 512:1024], resbuf[...], along, preferred_element_type=F32)
        line = a[0:1] + a[1:2] + a[2:3] + b[0:1] + b[1:2]
        dd[t] = jnp.zeros((8, 128), F32)
        dd[t, 0:1, :] = line[:, 0:128]
        dd[t, 1:2, :] = line[:, 128:256]

        def one(j, carry):
            send(dd.at[t], dd.at[t], dd_tx, dd_rx, rep_dev(r, wrap(t + j, 16)))
            return carry

        lax.fori_loop(1, 16, one, 0)

    def send_low(k, carry):
        dz = aim(k)

        @pl.when(k == 7)
        def _():
            zlin[14 + core] = zl[7, core]

        @pl.when(k < 7)
        def _():
            send(zl.at[k, core], zlin.at[2 * k + core], zl_tx, zl_rx, {"z": dz})

        send(zl.at[k, other], zlin.at[2 * k + core], zl_tx, zl_rx, {"z": dz, "c": other})
        return carry

    def flip(h):
        await_(zin.at[pl.ds(0, 8 - h)], zin_rx.at[h])
        v = zin[8 * h : 8 * h + 8].reshape(128, 512).astype(F32)
        for q in range(4):
            za[h, t, q] = v[:, q * 128 : (q + 1) * 128].T.astype(BF16)

    def gsend(h, g, a, b, dev, event):
        q = g["q"]
        tt = tcol(g, g[a], g[b])
        send(za.at[h, tt, q], za.at[h, tt, q], ag_tx, ag_rx.at[h, event], g[dev])

    def gwait(h, event):
        await_(za.at[h, 0], ag_rx.at[h, event])

    def ag1(h):
        for g in quarters:
            gsend(h, g, "a0", "b0", "dan", 0)
            gsend(h, g, "a0", "b0", "dao", 1)
        for g in quarters:
            gsend(h, g, "a0", "b0", "dbn", 3)
            gsend(h, g, "a0", "b0", "dbo", 7)

    def ag2(h):
        gwait(h, 0)
        for g in quarters:
            gsend(h, g, "ao", "b0", "dan", 2)
        for g in quarters:
            gsend(h, g, "ao", "b0", "dbn", 4)
        gwait(h, 1)
        for g in quarters:
            gsend(h, g, "an", "b0", "dbn", 5)
        for g in quarters:
            gsend(h, g, "ao", "b0", "dbo", 7)
            gsend(h, g, "an", "b0", "dbo", 7)

    def ag3(h):
        gwait(h, 3)
        for g in quarters:
            gsend(h, g, "a0", "bo", "dbn", 7)
        gwait(h, 2)
        for g in quarters:
            gsend(h, g, "af", "b0", "dbn", 6)
        for g in quarters:
            gsend(h, g, "af", "b0", "dbo", 7)

    def ag4part(h, i):
        gwait(h, 4 + i)
        for g in quarters:
            gsend(h, g, ("ao", "an", "af")[i], "bo", "dbn", 7)

    def ag4(h):
        for i in range(3):
            ag4part(h, i)

    def ag5(h):
        await_(za.at[h, pl.ds(0, 8)], ag_rx.at[h, 7])

    def on(n, parity, first, fn):
        k = (n - first) // 2

        @pl.when((lax.rem(n, 2) == parity) & (n >= first) & (n < first + 16))
        def _():
            fn(k)

    def step(n, carry):
        @pl.when(n == 12)
        def _():
            gathered()

        on(n, 0, 12, step_e)
        on(n, 1, 9, step_d)
        on(n, 0, 6, step_c)
        on(n, 1, 3, step_b)
        on(n, 0, 0, step_a)

        @pl.when(n == 0)
        def _():
            spread()

        @pl.when((n >= 1) & (n < 6))
        def _():
            pieces(n)

        @pl.when((n >= 5) & (lax.rem(n, 2) == 1))
        def _():
            ring((n - 5) // 2)

        @pl.when((n >= 13) & (n < 21))
        def _():
            project_head(n - 13)

        @pl.when(n == 22)
        def _():
            head_dots()

        @pl.when(n == 21)
        def _():
            flip(0)
            ag1(0)

        return carry

    lax.fori_loop(0, 27, step, 0)

    def absolute(lane):
        slot = lane >> 4
        k = slot >> 1
        m = 7 - (4 * ((k >> 1) & 1) + 2 * (k >> 2) + (k & 1))
        off = ((m + 1) >> 1) * (2 * (m & 1) - 1)
        return ((((zc + off + 8) & 7) * 2 + (slot & 1)) << 4) + (lane & 15)

    rows256 = lax.broadcasted_iota(jnp.int32, (256, 256), 0)
    cols256 = lax.broadcasted_iota(jnp.int32, (256, 256), 1)
    lane16 = lax.broadcasted_iota(jnp.int32, (16, 128), 1)
    row16 = lax.broadcasted_iota(jnp.int32, (16, 128), 0)
    pick = (lane16 & 15) == row16
    sa[r] = jnp.zeros((8, 128), F32)
    column = jnp.sum(acc[...], axis=1, keepdims=True)
    sa[r, 0:1, :] = jnp.sum(jnp.where(pick, column, 0.0), axis=0, keepdims=True)
    await_(dd.at[pl.ds(0, 15)], dd_rx)
    dots = jnp.sum(dd[...], axis=0)
    own_r = lax.broadcasted_iota(jnp.int32, (128, 128), 0)
    own_c = lax.broadcasted_iota(jnp.int32, (128, 128), 1)
    line = jnp.zeros((1, 128), F32)
    for h in range(2):
        own = ((own_r + 128 * h) == (t * 16 + (own_c & 15))).astype(F32)
        line = line + jnp.dot(dots, own, precision=HIGH, preferred_element_type=F32)[h : h + 1, :]
    sa[r, 1:2, :] = line

    def send_sa(j, carry):
        send(sa.at[r], sa.at[r], sa_tx, sa_rx, rep_dev(wrap(r + j, 16), t))
        return carry

    lax.fori_loop(1, 16, send_sa, 0)
    lax.fori_loop(0, 8, send_low, 0)
    ag2(0)
    flip(1)
    ag1(1)
    ag3(0)
    await_(sa.at[pl.ds(0, 15)], sa_rx)
    sb[t] = jnp.zeros((8, 128), F32)
    for i in range(2):
        for h in range(2):
            line = jnp.zeros((1, 128), F32)
            for j in range(8):
                line = line + jnp.where((lane16[0:1, :] >> 4) == j, sa[8 * h + j, i : i + 1, :], 0.0)
            sb[t, 2 * i + h : 2 * i + h + 1, :] = line

    def send_sb(j, carry):
        send(sb.at[t], sb.at[t], sb_tx, sb_rx, rep_dev(r, wrap(t + j, 16)))
        return carry

    lax.fori_loop(1, 16, send_sb, 0)
    ag2(1)
    ring(11)
    ag4(0)
    ring(12)
    ring(13)
    ag3(1)
    ag4part(1, 0)
    ag4part(1, 1)
    await_(smr.at[pl.ds(0, 15)], sm_rx)
    await_(sb.at[pl.ds(0, 15)], sb_rx)

    ints = smr[:, 0, :].astype(F32)
    tsub = lax.broadcasted_iota(jnp.int32, (16, 128), 0)
    lane = lax.broadcasted_iota(jnp.int32, (16, 128), 1)
    group_r = lax.broadcasted_iota(jnp.int32, (16, 128), 0)
    bl_r = lax.broadcasted_iota(jnp.int32, (128, 128), 0)
    bl_c = lax.broadcasted_iota(jnp.int32, (128, 128), 1)
    block = ((bl_r >> 4) == (bl_c >> 4)).astype(F32)
    eight = lax.broadcasted_iota(jnp.int32, (8, 128), 0)
    halves = []
    count = jnp.zeros((1, 1), F32)
    loss_sum = jnp.zeros((1, 1), F32)
    for h in range(2):
        spread = ((lane >> 4) + 8 * h == group_r).astype(F32)
        ex = lax.dot_general(ints, spread, (((0,), (0,)), ((), ())), precision=HIGH, preferred_element_type=F32)
        lens = [ex[i : i + 1, :] for i in range(4)]
        firsts = [ex[4 + i : 5 + i, :] for i in range(4)]
        seconds = [ex[8 + i : 9 + i, :] for i in range(4)]
        valid = [ex[12 + i : 13 + i, :] for i in range(4)]
        inv = 1.0 / jnp.sqrt(sb[:, h, :] / WIDTH + 1e-05)
        score = inv * sb[:, 2 + h, :]
        lens16 = jnp.zeros((16, 128), F32)
        for i in range(4):
            lens16 = lens16 + jnp.where((tsub >> 2) == i, lens[i], 0.0)
        within = ((tsub & 3) * 16 + (lane & 15)).astype(F32)
        live = (within < lens16).astype(F32)
        pooled = score * live
        stack = jnp.zeros((8, 128), F32)
        for i in range(4):
            part = jnp.sum(jnp.where((tsub >> 2) == i, pooled, 0.0), axis=0, keepdims=True)
            stack = stack + jnp.where(eight == i, part, 0.0)
        summed = jnp.dot(stack, block, precision=HIGH, preferred_element_type=F32)
        reward = [summed[i : i + 1, :] / lens[i] for i in range(4)]
        weights = []
        for p in range(4):
            margin = jnp.zeros((1, 128), F32)
            for i in range(4):
                margin = margin + jnp.where(firsts[p] == i, reward[i], 0.0) - jnp.where(seconds[p] == i, reward[i], 0.0)
            soft = jnp.maximum(-margin, 0.0) + jnp.log1p(jnp.exp(-jnp.abs(margin)))
            loss_sum = loss_sum + jnp.sum(valid[p] * soft, axis=1, keepdims=True) * (1.0 / 16.0)
            count = count + jnp.sum(valid[p], axis=1, keepdims=True) * (1.0 / 16.0)
            weights.append(valid[p] / (1.0 + jnp.exp(margin)))
        halves.append((lens, firsts, seconds, inv, score, live, weights))
    misc_ref[4:8, :] = jnp.broadcast_to(loss_sum / count, (4, 128))
    factor = -scale[0] / count
    for h in range(2):
        lens, firsts, seconds, inv, score, live, weights = halves[h]
        dscore = jnp.zeros((16, 128), F32)
        for i in range(4):
            d = jnp.zeros((1, 128), F32)
            for p in range(4):
                w = weights[p] * factor
                d = d + jnp.where(firsts[p] == i, w, 0.0) - jnp.where(seconds[p] == i, w, 0.0)
            dscore = dscore + jnp.where((tsub >> 2) == i, d / lens[i], 0.0)
        dscore = dscore * live
        ks[:, h * 128 : (h + 1) * 128] = inv * dscore
        cs[:, h * 128 : (h + 1) * 128] = inv * inv * dscore * score * (1.0 / WIDTH)
    to_slot = (rows256 == absolute(cols256)).astype(F32)
    kslot = jnp.dot(ks[...], to_slot, precision=HIGH, preferred_element_type=F32)
    cslot = jnp.dot(cs[...], to_slot, precision=HIGH, preferred_element_type=F32)
    for i in range(16):
        kc[i, 0:1, :] = kslot[i : i + 1, :]
        kc[i, 1:2, :] = cslot[i : i + 1, :]

    await_(zlin.at[pl.ds(0, 15)], zl_rx)
    krow = [kc[t, 0:1, 0:128], kc[t, 0:1, 128:256]]
    gsum = jnp.zeros((8, 128), F32)
    for q in range(4):
        row = jnp.zeros((1, 128), F32)
        for h in range(2):
            column = jnp.broadcast_to(krow[h], (128, 128)).T
            full = zin[8 * h : 8 * h + 8, :, q * 128 : (q + 1) * 128].astype(F32)
            full = full + zlin[8 * h : 8 * h + 8, :, q * 128 : (q + 1) * 128].astype(F32)
            row = row + jnp.sum(full.reshape(128, 128) * column, axis=0, keepdims=True)
        gsum = gsum + jnp.where(eight == q, row, 0.0)
    gmine[...] = gsum

    def send_g(j, carry):
        own = diag & (j == r)

        @pl.when(own)
        def _():
            gr[t] = gmine[...]

        @pl.when(jnp.logical_not(own))
        def _():
            send(gmine, gr.at[t], g_tx, g_rx, rep_dev(j, r))

        return carry

    lax.fori_loop(0, 16, send_g, 0)

    def contract(h, first):
        def group(gi, carry):
            if first:
                @pl.when(gi == 1)
                def _():
                    ag4part(1, 2)

            parts = []
            for j in range(4):
                tt = gi * 4 + j
                k1 = kc[tt, 0:1, h * 128 : (h + 1) * 128]
                c1 = kc[tt, 1:2, h * 128 : (h + 1) * 128]
                for q in range(4):
                    val = hgc[q] * k1 - za[h, tt, q].astype(F32) * c1
                    dt[q * 128 : (q + 1) * 128, j * 128 : (j + 1) * 128] = val.astype(BF16)
                rows = pl.ds(pl.multiple_of(tt * 16, 16), 16)
                for k in range(4 * h, 4 * h + 4):
                    parts.append(att[7 - (4 * (k // 2 % 2) + 2 * (k // 4) + k % 2), :, rows, :].reshape(32, 512))
            rhs = jnp.concatenate(parts, axis=0)
            prod = jnp.dot(dt[...], rhs, preferred_element_type=F32)

            if first:
                @pl.when(gi == 0)
                def _():
                    out_ref[...] = prod

                @pl.when(gi > 0)
                def _():
                    out_ref[...] += prod
            else:
                out_ref[...] += prod
            return carry

        lax.fori_loop(0, 4, group, 0)

    await_(att.at[pl.ds(0, 4), 0], att_rxc.at[0])
    await_(att.at[pl.ds(0, 4), 0], att_rxc.at[1])
    ag5(0)
    contract(0, True)
    ag5(1)
    contract(1, False)

    @pl.when(diag)
    def _():
        await_(gr.at[pl.ds(0, 15)], g_rx)
        await_(gr.at[pl.ds(0, 15)], g_tx)

    @pl.when(jnp.logical_not(diag))
    def _():
        await_(gr, g_rx)
        await_(gr, g_tx)

    misc_ref[0:4, :] = jnp.sum(gr[...], axis=0)[0:4, :]

    await_(rx.at[pl.ds(0, 15)], r1_tx)
    await_(vall.at[pl.ds(0, 15)], vec_tx)
    await_(zin.at[pl.ds(0, 8)], zin_tx.at[0])
    await_(zlin.at[pl.ds(0, 15)], zl_tx)
    await_(zin.at[pl.ds(0, 7)], zin_tx.at[1])
    await_(att.at[pl.ds(0, 7), 0], att_txz)
    await_(att.at[:, 0], att_txc)
    await_(smr.at[pl.ds(0, 15)], sm_tx)
    await_(sa.at[pl.ds(0, 15)], sa_tx)
    await_(dd.at[pl.ds(0, 15)], dd_tx)
    await_(sb.at[pl.ds(0, 15)], sb_tx)
    for i, buf in enumerate((m1s, m3s, m2s, n1s, n3s, n2s)):
        await_(buf, rs_tx.at[i])
    await_(za.at[:, pl.ds(0, 15)], ag_tx)


def shards(attn, out_weight, resid, norm_gain, head, lengths, pairs, pair_valid, loss_scale):
    vm = pltpu.VMEM
    stay = lambda a: pltpu.with_memory_space_constraint(a, pltpu.HBM)
    dma = pltpu.SemaphoreType.DMA
    big = (4, 8, 2, 4, 16, 128)
    little = (4, 8, 2, 16, 128)
    vspec = pl.BlockSpec(memory_space=pltpu.VMEM)
    anyspec = pl.BlockSpec(memory_space=pltpu.HBM)
    smem = pl.BlockSpec(memory_space=pltpu.SMEM)
    out, misc = pl.pallas_call(
        body,
        name="whole",
        out_shape=(jax.ShapeDtypeStruct((512, 512), F32), jax.ShapeDtypeStruct((8, 128), F32)),
        in_specs=[smem] + [anyspec] * 8,
        out_specs=(vspec, vspec),
        scratch_shapes=[
            pltpu.SMEM((4,), jnp.int32), pltpu.SMEM((2, 4), jnp.int32), pltpu.SMEM((4,), jnp.int32),
            vm((512,), BF16), vm((512,), BF16),
            vm((8, 2, 256, 512), BF16), vm((8, 1024, 512), BF16), vm((256, 512), BF16), vm((16, 16, 512), BF16),
            vm((8, 2, 16, 512), BF16), vm((16, 16, 512), BF16), vm((8, 2, 16, 512), BF16), vm((16, 16, 512), BF16), vm((8, 128), F32), vm((16, 8, 128), F32), vm((16, 4, 128), F32),
            vm((16, 128), F32), vm((8, 1024), F32), vm((8, 512), F32), vm((16, 8, 128), F32), vm((16, 8, 128), jnp.int32), vm((8, 2, 4, 4, 16, 512), F32),
            vm(big, BF16), vm(big, BF16), vm(big, BF16), vm(big, BF16), vm(big, BF16), vm(big, BF16), vm(big, F32),
            vm(little, BF16), vm(little, BF16), vm(little, BF16), vm(little, BF16), vm(little, BF16), vm(little, BF16),
            vm((2, 16, 4, 128, 128), BF16), vm((4, 128, 128), F32),
            vm((16, 8, 128), F32), vm((16, 8, 128), F32), vm((16, 256), F32), vm((16, 256), F32), vm((16, 8, 256), F32),
            vm((8, 128), F32), vm((16, 8, 128), F32), vm((512, 512), BF16),
            dma((2,)), dma((5,)), dma((8,)), dma, dma, dma((14,)), dma((2,)), dma, dma, dma((2,)), dma((2,)), dma, dma, dma, dma, dma, dma,
            dma((6,)), dma((6, 8)), dma, dma((2, 8)), dma, dma, dma, dma, dma, dma, dma, dma,
        ],
        compiler_params=pltpu.CompilerParams(collective_id=0, has_side_effects=True, vmem_limit_bytes=50 * 1024 * 1024),
    )(loss_scale, *(stay(a) for a in (lengths, pairs.T, pair_valid, attn, out_weight, resid, norm_gain, head)))
    g = misc[0:4].reshape(512)
    return (misc[4, 0:1], out, g * head.astype(F32), g * norm_gain.astype(F32))


def solution(mesh):
    finer = Mesh(mesh.devices.reshape(8, 2, 4, 4), ("z", "c", "x", "y"))
    rep, ten = ("z", "c"), ("x", "y")
    placed = (P(rep, ten), P(None, ten), P(rep, ten), P(ten), P(ten), P(rep), P(rep, None), P(rep), P())
    return jax.shard_map(
        shards,
        mesh=finer,
        in_specs=placed,
        out_specs=(P(), P(rep, ten), P(ten), P(ten)),
        check_vma=False,
    )
```

```python
import jax
import jax.numpy as jnp
from jax import lax
from jax.experimental import pallas as pl
from jax.experimental.pallas import tpu as pltpu
from jax.sharding import Mesh
from jax.sharding import PartitionSpec as P

F32 = jnp.float32
BF16 = jnp.bfloat16
MESH = pl.DeviceIdType.MESH
WIDTH = 8192
HIGH = lax.Precision.HIGHEST


def wrap(value, size):
    return lax.rem(value + size, size)


def body(scale, lens_hbm, pairs_hbm, valid_hbm, attn_hbm, w_hbm, resid_hbm, gain_hbm, head_hbm, out_ref, misc_ref,
         lens_ref, pairs_ref, valid_ref, gain_ref, head_ref, att, wbuf, resbuf, rx, zo, zin, zl, zlin, vec, vall, hgr, acc, hl, vsum, dd, smr, pf, m1s, m2s, m3s, m1r, m2r, m3r, s1f,
         n1s, n2s, n3s, n1r, n2r, n3r, za, hgc, sa, sb, ks, cs, kc, gmine, gr, dt,
         loc_sem, small_sem, w_sem, att_txz, att_txc, att_rx, att_rxc, r1_tx, r1_rx, zin_tx, zin_rx, zl_tx, zl_rx, vec_tx, vec_rx, sm_tx, sm_rx,
         rs_tx, rs_rx, ag_tx, ag_rx, sa_tx, sa_rx, sb_tx, sb_rx, g_tx, g_rx, dd_tx, dd_rx):
    zc, core, x, y = (lax.axis_index(n) for n in ("z", "c", "x", "y"))
    r = zc * 2 + core
    t = x * 4 + y
    other = 1 - core
    zp, zm = wrap(zc + 1, 8), wrap(zc - 1, 8)
    diag = r == t

    def rep_dev(rr, tt):
        return {"z": rr // 2, "c": lax.rem(rr, 2), "x": tt // 4, "y": lax.rem(tt, 4)}

    def send(src, dst, tx, rx, dev):
        pltpu.make_async_remote_copy(src_ref=src, dst_ref=dst, send_sem=tx, recv_sem=rx,
                                     device_id=dev, device_id_type=MESH).start()

    def await_(ref, sem):
        pltpu.make_async_copy(ref, ref, sem).wait()

    load_a = pltpu.make_async_copy(attn_hbm, att.at[0, core], loc_sem.at[0])
    load_r = pltpu.make_async_copy(resid_hbm, resbuf, loc_sem.at[1])
    load_a.start()
    loads = [
        pltpu.make_async_copy(a, b, small_sem.at[i])
        for i, (a, b) in enumerate((
            (lens_hbm, lens_ref), (pairs_hbm, pairs_ref), (valid_hbm, valid_ref), (gain_hbm, gain_ref), (head_hbm, head_ref)
        ))
    ]

    def place(k):
        return 7 - (4 * lax.rem(k // 2, 2) + 2 * (k // 4) + lax.rem(k, 2))

    def offset(k):
        m = place(k)
        return ((m + 1) // 2) * (2 * lax.rem(m, 2) - 1)

    def aim(k):
        return wrap(zc - offset(k), 8)

    def load_w(k, carry):
        rows = pl.ds(pl.multiple_of(aim(k) * 1024, 1024), 1024)
        pltpu.make_async_copy(w_hbm.at[rows], wbuf.at[k], w_sem.at[k]).start()
        return carry

    load_w(0, 0)

    barrier = pltpu.get_barrier_semaphore()

    def greet(j, carry):
        pl.semaphore_signal(barrier, 1, device_id=rep_dev(wrap(r + j, 16), t), device_id_type=MESH)
        pl.semaphore_signal(barrier, 1, device_id=rep_dev(r, wrap(t + j, 16)), device_id_type=MESH)
        return carry

    lax.fori_loop(1, 16, greet, 0)

    def greet2(j, carry):
        @pl.when(jnp.logical_not(diag & (j == t)))
        def _():
            pl.semaphore_signal(barrier, 1, device_id=rep_dev(t, j), device_id_type=MESH)

        @pl.when(jnp.logical_not(diag & (j == r)))
        def _():
            pl.semaphore_signal(barrier, 1, device_id=rep_dev(j, r), device_id_type=MESH)

        return carry

    lax.fori_loop(0, 16, greet2, 0)
    lax.fori_loop(1, 8, load_w, 0)
    load_r.start()
    for load in loads:
        load.start()
    load_a.wait()

    def multiply(k):
        await_(wbuf.at[k], w_sem.at[k])
        prod = lax.dot_general(att[0, core], wbuf[k], (((1,), (1,)), ((), ())), preferred_element_type=F32)
        pf[k, 0] = prod[:, 0:512].reshape(4, 4, 16, 512)
        pf[k, 1] = prod[:, 512:1024].reshape(4, 4, 16, 512)

    multiply(0)
    pl.semaphore_wait(barrier, jnp.where(diag, 60, 62))

    def rows_of(j):
        return pl.ds(pl.multiple_of(j * 64, 64), 64)

    def up(k, j):
        return att.at[k, core, rows_of(lax.rem(j + 2, 4))]

    def down(k, j):
        return att.at[k, core, rows_of(j)]

    def send_own(j, carry):
        send(up(0, j), up(1, j), att_txz, att_rx.at[j], {"z": zm})
        send(down(0, j), down(2, j), att_txz, att_rx.at[j], {"z": zp})
        return carry

    lax.fori_loop(0, 4, send_own, 0)
    send(att.at[0, core], att.at[0, core], att_txc, att_rxc.at[1], {"c": other})

    def spread():
        for load in loads:
            load.wait()
        lane8 = lax.broadcasted_iota(jnp.int32, (8, 128), 1)
        ints8 = jnp.zeros((8, 128), jnp.int32)
        for i in range(4):
            ints8 = jnp.where(lane8 == i, lens_ref[i], ints8)
            ints8 = jnp.where(lane8 == 4 + i, pairs_ref[0, i], ints8)
            ints8 = jnp.where(lane8 == 8 + i, pairs_ref[1, i], ints8)
            ints8 = jnp.where(lane8 == 12 + i, valid_ref[i], ints8)
        smr[r] = ints8
        vec[0:4, :] = gain_ref[...].astype(F32).reshape(4, 128)
        vec[4:8, :] = head_ref[...].astype(F32).reshape(4, 128)
        vall[t] = vec[...]
        load_r.wait()
        rx[t] = resbuf[pl.ds(pl.multiple_of(t * 16, 16), 16), :]
        acc[...] = jnp.zeros((16, 128), F32)
        hl[...] = jnp.zeros((8, 1024), F32)
        vsum[...] = jnp.zeros((8, 512), F32)

    def pieces(n):
        def one(j, carry):
            tt = wrap(t + j, 16)
            rows = pl.ds(pl.multiple_of(tt * 16, 16), 16)
            send(smr.at[r], smr.at[r], sm_tx, sm_rx, rep_dev(wrap(r + j, 16), t))
            send(vec, vall.at[t], vec_tx, vec_rx, rep_dev(r, tt))
            send(resbuf.at[rows, :], rx.at[t], r1_tx, r1_rx, rep_dev(r, tt))
            return carry

        lax.fori_loop(3 * n - 2, 3 * n + 1, one, 0)

    def gathered():
        await_(vall.at[pl.ds(0, 15)], vec_rx)
        await_(rx.at[pl.ds(0, 15)], r1_rx)
        hgr[...] = vall[:, 0:4, :] * vall[:, 4:8, :]
        for q in range(4):
            hgc[q] = jnp.broadcast_to(hgr[r, q : q + 1, :], (128, 128)).T

    quarters = []
    for q in range(4):
        first = "x" if q < 2 else "y"
        second = "y" if q < 2 else "x"
        a0, b0 = (x, y) if q < 2 else (y, x)
        s = 1 if q % 2 == 0 else -1
        quarters.append(dict(
            q=q, a0=a0, b0=b0, lanes=slice(q * 128, (q + 1) * 128),
            af=wrap(a0 + 2, 4), an=wrap(a0 + s, 4), ao=wrap(a0 - s, 4),
            bf=wrap(b0 + 2, 4), bn=wrap(b0 + s, 4), bo=wrap(b0 - s, 4),
            dan={first: wrap(a0 + s, 4)}, dao={first: wrap(a0 - s, 4)},
            dbn={second: wrap(b0 + s, 4)}, dbo={second: wrap(b0 - s, 4)},
        ))

    def chunk(k, g, a):
        if g["q"] < 2:
            v = pf[k, :, pl.ds(a, 1), :, :, g["lanes"]]
        else:
            v = pf[k, :, :, pl.ds(a, 1), :, g["lanes"]]
        return v.reshape(2, 4, 16, 128)

    def tcol(g, a, b):
        return a * 4 + b if g["q"] < 2 else b * 4 + a

    def ring(n):
        n = jnp.int32(n)
        d, j = n // 4 + 1, lax.rem(n, 4)
        kp, km = 2 * d - 1, 2 * d
        await_(att.at[0, core, pl.ds(0, 128)], att_rx.at[n])

        @pl.when(n < 10)
        def _():
            send(up(kp, j), up(jnp.minimum(kp + 2, 7), j), att_txz, att_rx.at[n + 4], {"z": zm})
            send(down(km, j), down(jnp.minimum(km + 2, 7), j), att_txz, att_rx.at[n + 4], {"z": zp})

        @pl.when((j == 3) & (n < 12))
        def _():
            h = jnp.where((kp == 3) | (kp == 7), 0, 1)
            send(att.at[kp, core], att.at[kp, core], att_txc, att_rxc.at[h], {"c": other})
            h = jnp.where((km == 2) | (km == 6), 0, 1)
            send(att.at[km, core], att.at[km, core], att_txc, att_rxc.at[h], {"c": other})

        @pl.when(n == 13)
        def _():
            send(att.at[7, core], att.at[7, core], att_txc, att_rxc.at[0], {"c": other})

    def step_a(k):
        @pl.when(k > 0)
        def _():
            multiply(k)

        for g in quarters:
            q = g["q"]
            m1s[q, k] = chunk(k, g, g["af"]).astype(BF16)
            send(m1s.at[q, k], m1r.at[q, k], rs_tx.at[0], rs_rx.at[0, k], g["dan"])
        for g in quarters:
            q = g["q"]
            m3s[q, k] = chunk(k, g, g["ao"]).astype(BF16)
            send(m3s.at[q, k], m3r.at[q, k], rs_tx.at[1], rs_rx.at[1, k], g["dao"])

    def step_b(k):
        await_(m1r.at[:, k], rs_rx.at[0, k])
        for g in quarters:
            q = g["q"]
            m2s[q, k] = (chunk(k, g, g["an"]) + m1r[q, k].astype(F32)).astype(BF16)
            send(m2s.at[q, k], m2r.at[q, k], rs_tx.at[2], rs_rx.at[2, k], g["dan"])

    def step_c(k):
        await_(m3r.at[:, k], rs_rx.at[1, k])
        await_(m2r.at[:, k], rs_rx.at[2, k])
        for g in quarters:
            q = g["q"]
            s1f[q, k] = chunk(k, g, g["a0"]) + m2r[q, k].astype(F32) + m3r[q, k].astype(F32)
            n1s[q, k] = s1f[q, k, :, pl.ds(g["bf"], 1)].reshape(2, 16, 128).astype(BF16)
            send(n1s.at[q, k], n1r.at[q, k], rs_tx.at[3], rs_rx.at[3, k], g["dbn"])
            n3s[q, k] = s1f[q, k, :, pl.ds(g["bo"], 1)].reshape(2, 16, 128).astype(BF16)
            send(n3s.at[q, k], n3r.at[q, k], rs_tx.at[4], rs_rx.at[4, k], g["dbo"])

    def step_d(k):
        await_(n1r.at[:, k], rs_rx.at[3, k])
        for g in quarters:
            q = g["q"]
            n2s[q, k] = (s1f[q, k, :, pl.ds(g["bn"], 1)].reshape(2, 16, 128) + n1r[q, k].astype(F32)).astype(BF16)
            send(n2s.at[q, k], n2r.at[q, k], rs_tx.at[5], rs_rx.at[5, k], g["dbn"])

    def step_e(k):
        dz = aim(k)
        sq = jnp.zeros((16, 128), F32)
        await_(n2r.at[:, k], rs_rx.at[5, k])
        await_(n3r.at[:, k], rs_rx.at[4, k])
        for g in quarters:
            q = g["q"]
            total = s1f[q, k, :, pl.ds(g["b0"], 1)].reshape(2, 16, 128) + n2r[q, k].astype(F32) + n3r[q, k].astype(F32)
            total = total + rx[pl.ds(2 * dz, 2), :, g["lanes"]].astype(F32)
            for cc in range(2):
                sq = sq + total[cc] * total[cc]
            high = total.astype(BF16)
            zo[k, :, :, g["lanes"]] = high
            zl[k, :, :, g["lanes"]] = (total - high.astype(F32)).astype(BF16)
        acc[...] += sq
        h = k // 4

        @pl.when(k == 7)
        def _():
            zin[14 + core] = zo[7, core]

        @pl.when(k < 7)
        def _():
            send(zo.at[k, core], zin.at[2 * k + core], zin_tx.at[h], zin_rx.at[h], {"z": dz})

        send(zo.at[k, other], zin.at[2 * k + core], zin_tx.at[h], zin_rx.at[h], {"z": dz, "c": other})

    def halves_of(row):
        high = row.astype(BF16).astype(F32)
        return high, row - high

    def project_head(k):
        for cc in range(2):
            for q in range(4):
                at = slice((cc * 4 + q) * 128, (cc * 4 + q + 1) * 128)
                high, low = halves_of(hgr[2 * aim(k) + cc, q : q + 1, :])
                hl[0:1, at] = high
                hl[1:2, at] = low
        vsum[...] += jnp.dot(hl[...].astype(BF16), wbuf[k], preferred_element_type=F32)

    def head_dots():
        high, rest = halves_of(vsum[0:1, :] + vsum[1:2, :])
        middle, low = halves_of(rest)
        hl[0:1, 0:512] = high
        hl[1:2, 0:512] = middle
        hl[2:3, 0:512] = low
        for q in range(4):
            at = slice(512 + q * 128, 640 + q * 128)
            high, low = halves_of(hgr[t, q : q + 1, :])
            hl[0:1, at] = high
            hl[1:2, at] = low
        rows = hl[...].astype(BF16)
        along = (((1,), (1,)), ((), ()))
        a = lax.dot_general(rows[:, 0:512], att[0, core], along, preferred_element_type=F32)
        b = lax.dot_general(rows[:, 512:1024], resbuf[...], along, preferred_element_type=F32)
        line = a[0:1] + a[1:2] + a[2:3] + b[0:1] + b[1:2]
        dd[t] = jnp.zeros((8, 128), F32)
        dd[t, 0:1, :] = line[:, 0:128]
        dd[t, 1:2, :] = line[:, 128:256]

        def one(j, carry):
            send(dd.at[t], dd.at[t], dd_tx, dd_rx, rep_dev(r, wrap(t + j, 16)))
            return carry

        lax.fori_loop(1, 16, one, 0)

    def send_low(k, carry):
        dz = aim(k)

        @pl.when(k == 7)
        def _():
            zlin[14 + core] = zl[7, core]

        @pl.when(k < 7)
        def _():
            send(zl.at[k, core], zlin.at[2 * k + core], zl_tx, zl_rx, {"z": dz})

        send(zl.at[k, other], zlin.at[2 * k + core], zl_tx, zl_rx, {"z": dz, "c": other})
        return carry

    def flip(h):
        await_(zin.at[pl.ds(0, 8 - h)], zin_rx.at[h])
        v = zin[8 * h : 8 * h + 8].reshape(128, 512).astype(F32)
        for q in range(4):
            za[h, t, q] = v[:, q * 128 : (q + 1) * 128].T.astype(BF16)

    def gsend(h, g, a, b, dev, event):
        q = g["q"]
        tt = tcol(g, g[a], g[b])
        send(za.at[h, tt, q], za.at[h, tt, q], ag_tx, ag_rx.at[h, event], g[dev])

    def gwait(h, event):
        await_(za.at[h, 0], ag_rx.at[h, event])

    def ag1(h):
        for g in quarters:
            gsend(h, g, "a0", "b0", "dan", 0)
            gsend(h, g, "a0", "b0", "dao", 1)
        for g in quarters:
            gsend(h, g, "a0", "b0", "dbn", 3)
            gsend(h, g, "a0", "b0", "dbo", 7)

    def ag2(h):
        gwait(h, 0)
        for g in quarters:
            gsend(h, g, "ao", "b0", "dan", 2)
        for g in quarters:
            gsend(h, g, "ao", "b0", "dbn", 4)
        gwait(h, 1)
        for g in quarters:
            gsend(h, g, "an", "b0", "dbn", 5)
        for g in quarters:
            gsend(h, g, "ao", "b0", "dbo", 7)
            gsend(h, g, "an", "b0", "dbo", 7)

    def ag3(h):
        gwait(h, 3)
        for g in quarters:
            gsend(h, g, "a0", "bo", "dbn", 7)
        gwait(h, 2)
        for g in quarters:
            gsend(h, g, "af", "b0", "dbn", 6)
        for g in quarters:
            gsend(h, g, "af", "b0", "dbo", 7)

    def ag4part(h, i):
        gwait(h, 4 + i)
        for g in quarters:
            gsend(h, g, ("ao", "an", "af")[i], "bo", "dbn", 7)

    def ag4(h):
        for i in range(3):
            ag4part(h, i)

    def ag5(h):
        await_(za.at[h, pl.ds(0, 8)], ag_rx.at[h, 7])

    def on(n, parity, first, fn):
        k = (n - first) // 2

        @pl.when((lax.rem(n, 2) == parity) & (n >= first) & (n < first + 16))
        def _():
            fn(k)

    def step(n, carry):
        @pl.when(n == 12)
        def _():
            gathered()

        on(n, 0, 12, step_e)
        on(n, 1, 9, step_d)
        on(n, 0, 6, step_c)
        on(n, 1, 3, step_b)
        on(n, 0, 0, step_a)

        @pl.when(n == 0)
        def _():
            spread()

        @pl.when((n >= 1) & (n < 6))
        def _():
            pieces(n)

        @pl.when((n >= 5) & (lax.rem(n, 2) == 1))
        def _():
            ring((n - 5) // 2)

        @pl.when((n >= 13) & (n < 21))
        def _():
            project_head(n - 13)

        @pl.when(n == 22)
        def _():
            head_dots()

        @pl.when(n == 21)
        def _():
            flip(0)
            ag1(0)

        return carry

    lax.fori_loop(0, 27, step, 0)

    def absolute(lane):
        slot = lane >> 4
        k = slot >> 1
        m = 7 - (4 * ((k >> 1) & 1) + 2 * (k >> 2) + (k & 1))
        off = ((m + 1) >> 1) * (2 * (m & 1) - 1)
        return ((((zc + off + 8) & 7) * 2 + (slot & 1)) << 4) + (lane & 15)

    rows256 = lax.broadcasted_iota(jnp.int32, (256, 256), 0)
    cols256 = lax.broadcasted_iota(jnp.int32, (256, 256), 1)
    lane16 = lax.broadcasted_iota(jnp.int32, (16, 128), 1)
    row16 = lax.broadcasted_iota(jnp.int32, (16, 128), 0)
    pick = (lane16 & 15) == row16
    sa[r] = jnp.zeros((8, 128), F32)
    ag2(0)
    flip(1)
    ag1(1)
    column = jnp.sum(acc[...], axis=1, keepdims=True)
    sa[r, 0:1, :] = jnp.sum(jnp.where(pick, column, 0.0), axis=0, keepdims=True)
    await_(dd.at[pl.ds(0, 15)], dd_rx)
    dots = jnp.sum(dd[...], axis=0)
    own_r = lax.broadcasted_iota(jnp.int32, (128, 128), 0)
    own_c = lax.broadcasted_iota(jnp.int32, (128, 128), 1)
    line = jnp.zeros((1, 128), F32)
    for h in range(2):
        own = ((own_r + 128 * h) == (t * 16 + (own_c & 15))).astype(F32)
        line = line + jnp.dot(dots, own, precision=HIGH, preferred_element_type=F32)[h : h + 1, :]
    sa[r, 1:2, :] = line

    def send_sa(j, carry):
        send(sa.at[r], sa.at[r], sa_tx, sa_rx, rep_dev(wrap(r + j, 16), t))
        return carry

    lax.fori_loop(1, 16, send_sa, 0)
    lax.fori_loop(0, 8, send_low, 0)
    ag3(0)
    await_(sa.at[pl.ds(0, 15)], sa_rx)
    sb[t] = jnp.zeros((8, 128), F32)
    for i in range(2):
        for h in range(2):
            line = jnp.zeros((1, 128), F32)
            for j in range(8):
                line = line + jnp.where((lane16[0:1, :] >> 4) == j, sa[8 * h + j, i : i + 1, :], 0.0)
            sb[t, 2 * i + h : 2 * i + h + 1, :] = line

    def send_sb(j, carry):
        send(sb.at[t], sb.at[t], sb_tx, sb_rx, rep_dev(r, wrap(t + j, 16)))
        return carry

    lax.fori_loop(1, 16, send_sb, 0)
    ag2(1)
    ring(11)
    ag4(0)
    ring(12)
    ring(13)
    ag3(1)
    ag4part(1, 0)
    ag4part(1, 1)
    await_(smr.at[pl.ds(0, 15)], sm_rx)
    await_(sb.at[pl.ds(0, 15)], sb_rx)

    ints = smr[:, 0, :].astype(F32)
    tsub = lax.broadcasted_iota(jnp.int32, (16, 128), 0)
    lane = lax.broadcasted_iota(jnp.int32, (16, 128), 1)
    group_r = lax.broadcasted_iota(jnp.int32, (16, 128), 0)
    bl_r = lax.broadcasted_iota(jnp.int32, (128, 128), 0)
    bl_c = lax.broadcasted_iota(jnp.int32, (128, 128), 1)
    block = ((bl_r >> 4) == (bl_c >> 4)).astype(F32)
    eight = lax.broadcasted_iota(jnp.int32, (8, 128), 0)
    halves = []
    count = jnp.zeros((1, 1), F32)
    loss_sum = jnp.zeros((1, 1), F32)
    for h in range(2):
        spread = ((lane >> 4) + 8 * h == group_r).astype(F32)
        ex = lax.dot_general(ints, spread, (((0,), (0,)), ((), ())), precision=HIGH, preferred_element_type=F32)
        lens = [ex[i : i + 1, :] for i in range(4)]
        firsts = [ex[4 + i : 5 + i, :] for i in range(4)]
        seconds = [ex[8 + i : 9 + i, :] for i in range(4)]
        valid = [ex[12 + i : 13 + i, :] for i in range(4)]
        inv = 1.0 / jnp.sqrt(sb[:, h, :] / WIDTH + 1e-05)
        score = inv * sb[:, 2 + h, :]
        lens16 = jnp.zeros((16, 128), F32)
        for i in range(4):
            lens16 = lens16 + jnp.where((tsub >> 2) == i, lens[i], 0.0)
        within = ((tsub & 3) * 16 + (lane & 15)).astype(F32)
        live = (within < lens16).astype(F32)
        pooled = score * live
        stack = jnp.zeros((8, 128), F32)
        for i in range(4):
            part = jnp.sum(jnp.where((tsub >> 2) == i, pooled, 0.0), axis=0, keepdims=True)
            stack = stack + jnp.where(eight == i, part, 0.0)
        summed = jnp.dot(stack, block, precision=HIGH, preferred_element_type=F32)
        reward = [summed[i : i + 1, :] / lens[i] for i in range(4)]
        weights = []
        for p in range(4):
            margin = jnp.zeros((1, 128), F32)
            for i in range(4):
                margin = margin + jnp.where(firsts[p] == i, reward[i], 0.0) - jnp.where(seconds[p] == i, reward[i], 0.0)
            soft = jnp.maximum(-margin, 0.0) + jnp.log1p(jnp.exp(-jnp.abs(margin)))
            loss_sum = loss_sum + jnp.sum(valid[p] * soft, axis=1, keepdims=True) * (1.0 / 16.0)
            count = count + jnp.sum(valid[p], axis=1, keepdims=True) * (1.0 / 16.0)
            weights.append(valid[p] / (1.0 + jnp.exp(margin)))
        halves.append((lens, firsts, seconds, inv, score, live, weights))
    misc_ref[4:8, :] = jnp.broadcast_to(loss_sum / count, (4, 128))
    factor = -scale[0] / count
    for h in range(2):
        lens, firsts, seconds, inv, score, live, weights = halves[h]
        dscore = jnp.zeros((16, 128), F32)
        for i in range(4):
            d = jnp.zeros((1, 128), F32)
            for p in range(4):
                w = weights[p] * factor
                d = d + jnp.where(firsts[p] == i, w, 0.0) - jnp.where(seconds[p] == i, w, 0.0)
            dscore = dscore + jnp.where((tsub >> 2) == i, d / lens[i], 0.0)
        dscore = dscore * live
        ks[:, h * 128 : (h + 1) * 128] = inv * dscore
        cs[:, h * 128 : (h + 1) * 128] = inv * inv * dscore * score * (1.0 / WIDTH)
    to_slot = (rows256 == absolute(cols256)).astype(F32)
    kslot = jnp.dot(ks[...], to_slot, precision=HIGH, preferred_element_type=F32)
    cslot = jnp.dot(cs[...], to_slot, precision=HIGH, preferred_element_type=F32)
    for i in range(16):
        kc[i, 0:1, :] = kslot[i : i + 1, :]
        kc[i, 1:2, :] = cslot[i : i + 1, :]

    await_(zlin.at[pl.ds(0, 15)], zl_rx)
    krow = [kc[t, 0:1, 0:128], kc[t, 0:1, 128:256]]
    gsum = jnp.zeros((8, 128), F32)
    for q in range(4):
        row = jnp.zeros((1, 128), F32)
        for h in range(2):
            column = jnp.broadcast_to(krow[h], (128, 128)).T
            full = zin[8 * h : 8 * h + 8, :, q * 128 : (q + 1) * 128].astype(F32)
            full = full + zlin[8 * h : 8 * h + 8, :, q * 128 : (q + 1) * 128].astype(F32)
            row = row + jnp.sum(full.reshape(128, 128) * column, axis=0, keepdims=True)
        gsum = gsum + jnp.where(eight == q, row, 0.0)
    gmine[...] = gsum

    def send_g(j, carry):
        own = diag & (j == r)

        @pl.when(own)
        def _():
            gr[t] = gmine[...]

        @pl.when(jnp.logical_not(own))
        def _():
            send(gmine, gr.at[t], g_tx, g_rx, rep_dev(j, r))

        return carry

    lax.fori_loop(0, 16, send_g, 0)

    def contract(h, first):
        def group(gi, carry):
            if first:
                @pl.when(gi == 1)
                def _():
                    ag4part(1, 2)

            parts = []
            for j in range(8):
                tt = gi * 8 + j
                k1 = kc[tt, 0:1, h * 128 : (h + 1) * 128]
                c1 = kc[tt, 1:2, h * 128 : (h + 1) * 128]
                for q in range(4):
                    val = hgc[q] * k1 - za[h, tt, q].astype(F32) * c1
                    dt[q * 128 : (q + 1) * 128, j * 128 : (j + 1) * 128] = val.astype(BF16)
                rows = pl.ds(pl.multiple_of(tt * 16, 16), 16)
                for k in range(4 * h, 4 * h + 4):
                    parts.append(att[7 - (4 * (k // 2 % 2) + 2 * (k // 4) + k % 2), :, rows, :].reshape(32, 512))
            rhs = jnp.concatenate(parts, axis=0)
            prod = jnp.dot(dt[...], rhs, preferred_element_type=F32)

            if first:
                @pl.when(gi == 0)
                def _():
                    out_ref[...] = prod

                @pl.when(gi > 0)
                def _():
                    out_ref[...] += prod
            else:
                out_ref[...] += prod
            return carry

        lax.fori_loop(0, 2, group, 0)

    await_(att.at[pl.ds(0, 4), 0], att_rxc.at[0])
    await_(att.at[pl.ds(0, 4), 0], att_rxc.at[1])
    ag5(0)
    contract(0, True)
    ag5(1)
    contract(1, False)

    @pl.when(diag)
    def _():
        await_(gr.at[pl.ds(0, 15)], g_rx)
        await_(gr.at[pl.ds(0, 15)], g_tx)

    @pl.when(jnp.logical_not(diag))
    def _():
        await_(gr, g_rx)
        await_(gr, g_tx)

    misc_ref[0:4, :] = jnp.sum(gr[...], axis=0)[0:4, :]

    await_(rx.at[pl.ds(0, 15)], r1_tx)
    await_(vall.at[pl.ds(0, 15)], vec_tx)
    await_(zin.at[pl.ds(0, 8)], zin_tx.at[0])
    await_(zlin.at[pl.ds(0, 15)], zl_tx)
    await_(zin.at[pl.ds(0, 7)], zin_tx.at[1])
    await_(att.at[pl.ds(0, 7), 0], att_txz)
    await_(att.at[:, 0], att_txc)
    await_(smr.at[pl.ds(0, 15)], sm_tx)
    await_(sa.at[pl.ds(0, 15)], sa_tx)
    await_(dd.at[pl.ds(0, 15)], dd_tx)
    await_(sb.at[pl.ds(0, 15)], sb_tx)
    for i, buf in enumerate((m1s, m3s, m2s, n1s, n3s, n2s)):
        await_(buf, rs_tx.at[i])
    await_(za.at[:, pl.ds(0, 15)], ag_tx)


def shards(attn, out_weight, resid, norm_gain, head, lengths, pairs, pair_valid, loss_scale):
    vm = pltpu.VMEM
    stay = lambda a: pltpu.with_memory_space_constraint(a, pltpu.HBM)
    dma = pltpu.SemaphoreType.DMA
    big = (4, 8, 2, 4, 16, 128)
    little = (4, 8, 2, 16, 128)
    vspec = pl.BlockSpec(memory_space=pltpu.VMEM)
    anyspec = pl.BlockSpec(memory_space=pltpu.HBM)
    smem = pl.BlockSpec(memory_space=pltpu.SMEM)
    out, misc = pl.pallas_call(
        body,
        name="whole",
        out_shape=(jax.ShapeDtypeStruct((512, 512), F32), jax.ShapeDtypeStruct((8, 128), F32)),
        in_specs=[smem] + [anyspec] * 8,
        out_specs=(vspec, vspec),
        scratch_shapes=[
            pltpu.SMEM((4,), jnp.int32), pltpu.SMEM((2, 4), jnp.int32), pltpu.SMEM((4,), jnp.int32),
            vm((512,), BF16), vm((512,), BF16),
            vm((8, 2, 256, 512), BF16), vm((8, 1024, 512), BF16), vm((256, 512), BF16), vm((16, 16, 512), BF16),
            vm((8, 2, 16, 512), BF16), vm((16, 16, 512), BF16), vm((8, 2, 16, 512), BF16), vm((16, 16, 512), BF16), vm((8, 128), F32), vm((16, 8, 128), F32), vm((16, 4, 128), F32),
            vm((16, 128), F32), vm((8, 1024), F32), vm((8, 512), F32), vm((16, 8, 128), F32), vm((16, 8, 128), jnp.int32), vm((8, 2, 4, 4, 16, 512), F32),
            vm(big, BF16), vm(big, BF16), vm(big, BF16), vm(big, BF16), vm(big, BF16), vm(big, BF16), vm(big, F32),
            vm(little, BF16), vm(little, BF16), vm(little, BF16), vm(little, BF16), vm(little, BF16), vm(little, BF16),
            vm((2, 16, 4, 128, 128), BF16), vm((4, 128, 128), F32),
            vm((16, 8, 128), F32), vm((16, 8, 128), F32), vm((16, 256), F32), vm((16, 256), F32), vm((16, 8, 256), F32),
            vm((8, 128), F32), vm((16, 8, 128), F32), vm((512, 1024), BF16),
            dma((2,)), dma((5,)), dma((8,)), dma, dma, dma((14,)), dma((2,)), dma, dma, dma((2,)), dma((2,)), dma, dma, dma, dma, dma, dma,
            dma((6,)), dma((6, 8)), dma, dma((2, 8)), dma, dma, dma, dma, dma, dma, dma, dma,
        ],
        compiler_params=pltpu.CompilerParams(collective_id=0, has_side_effects=True, vmem_limit_bytes=50 * 1024 * 1024),
    )(loss_scale, *(stay(a) for a in (lengths, pairs.T, pair_valid, attn, out_weight, resid, norm_gain, head)))
    g = misc[0:4].reshape(512)
    return (misc[4, 0:1], out, g * head.astype(F32), g * norm_gain.astype(F32))


def solution(mesh):
    finer = Mesh(mesh.devices.reshape(8, 2, 4, 4), ("z", "c", "x", "y"))
    rep, ten = ("z", "c"), ("x", "y")
    placed = (P(rep, ten), P(None, ten), P(rep, ten), P(ten), P(ten), P(rep), P(rep, None), P(rep), P())
    return jax.shard_map(
        shards,
        mesh=finer,
        in_specs=placed,
        out_specs=(P(), P(rep, ten), P(ten), P(ten)),
        check_vma=False,
    )
```

```python
import jax
import jax.numpy as jnp
from jax import lax
from jax.experimental import pallas as pl
from jax.experimental.pallas import tpu as pltpu
from jax.sharding import Mesh
from jax.sharding import PartitionSpec as P

F32 = jnp.float32
BF16 = jnp.bfloat16
MESH = pl.DeviceIdType.MESH
WIDTH = 8192
HIGH = lax.Precision.HIGHEST


def wrap(value, size):
    return lax.rem(value + size, size)


def body(scale, lens_hbm, pairs_hbm, valid_hbm, attn_hbm, w_hbm, resid_hbm, gain_hbm, head_hbm, out_ref, misc_ref,
         lens_ref, pairs_ref, valid_ref, gain_ref, head_ref, att, wbuf, resbuf, rx, zo, zin, zl, zlin, vec, vall, hgr, acc, hl, vsum, dd, smr, pf, m1s, m2s, m3s, m1r, m2r, m3r, s1f,
         n1s, n2s, n3s, n1r, n2r, n3r, za, hgc, sa, sb, ks, cs, kc, gmine, gr, dt,
         loc_sem, small_sem, w_sem, att_txz, att_txc, att_rx, att_rxc, r1_tx, r1_rx, zin_tx, zin_rx, zl_tx, zl_rx, vec_tx, vec_rx, sm_tx, sm_rx,
         rs_tx, rs_rx, ag_tx, ag_rx, sa_tx, sa_rx, sb_tx, sb_rx, g_tx, g_rx, dd_tx, dd_rx):
    zc, core, x, y = (lax.axis_index(n) for n in ("z", "c", "x", "y"))
    r = zc * 2 + core
    t = x * 4 + y
    other = 1 - core
    zp, zm = wrap(zc + 1, 8), wrap(zc - 1, 8)
    diag = r == t

    def rep_dev(rr, tt):
        return {"z": rr // 2, "c": lax.rem(rr, 2), "x": tt // 4, "y": lax.rem(tt, 4)}

    def send(src, dst, tx, rx, dev):
        pltpu.make_async_remote_copy(src_ref=src, dst_ref=dst, send_sem=tx, recv_sem=rx,
                                     device_id=dev, device_id_type=MESH).start()

    def await_(ref, sem):
        pltpu.make_async_copy(ref, ref, sem).wait()

    load_a = pltpu.make_async_copy(attn_hbm, att.at[0, core], loc_sem.at[0])
    load_r = pltpu.make_async_copy(resid_hbm, resbuf, loc_sem.at[1])
    load_a.start()
    loads = [
        pltpu.make_async_copy(a, b, small_sem.at[i])
        for i, (a, b) in enumerate((
            (lens_hbm, lens_ref), (pairs_hbm, pairs_ref), (valid_hbm, valid_ref), (gain_hbm, gain_ref), (head_hbm, head_ref)
        ))
    ]

    def place(k):
        return 7 - (4 * lax.rem(k // 2, 2) + 2 * (k // 4) + lax.rem(k, 2))

    def offset(k):
        m = place(k)
        return ((m + 1) // 2) * (2 * lax.rem(m, 2) - 1)

    def aim(k):
        return wrap(zc - offset(k), 8)

    def load_w(k, carry):
        rows = pl.ds(pl.multiple_of(aim(k) * 1024, 1024), 1024)
        pltpu.make_async_copy(w_hbm.at[rows], wbuf.at[k], w_sem.at[k]).start()
        return carry

    load_w(0, 0)

    barrier = pltpu.get_barrier_semaphore()

    def greet(j, carry):
        pl.semaphore_signal(barrier, 1, device_id=rep_dev(wrap(r + j, 16), t), device_id_type=MESH)
        pl.semaphore_signal(barrier, 1, device_id=rep_dev(r, wrap(t + j, 16)), device_id_type=MESH)
        return carry

    lax.fori_loop(1, 16, greet, 0)

    def greet2(j, carry):
        @pl.when(jnp.logical_not(diag & (j == t)))
        def _():
            pl.semaphore_signal(barrier, 1, device_id=rep_dev(t, j), device_id_type=MESH)

        @pl.when(jnp.logical_not(diag & (j == r)))
        def _():
            pl.semaphore_signal(barrier, 1, device_id=rep_dev(j, r), device_id_type=MESH)

        return carry

    lax.fori_loop(0, 16, greet2, 0)
    lax.fori_loop(1, 8, load_w, 0)
    load_r.start()
    for load in loads:
        load.start()
    load_a.wait()

    def multiply(k):
        await_(wbuf.at[k], w_sem.at[k])
        prod = lax.dot_general(att[0, core], wbuf[k], (((1,), (1,)), ((), ())), preferred_element_type=F32)
        pf[k, 0] = prod[:, 0:512].reshape(4, 4, 16, 512)
        pf[k, 1] = prod[:, 512:1024].reshape(4, 4, 16, 512)

    multiply(0)
    pl.semaphore_wait(barrier, jnp.where(diag, 60, 62))

    def rows_of(j):
        return pl.ds(pl.multiple_of(j * 64, 64), 64)

    def up(k, j):
        return att.at[k, core, rows_of(lax.rem(j + 2, 4))]

    def down(k, j):
        return att.at[k, core, rows_of(j)]

    def send_own(j, carry):
        send(up(0, j), up(1, j), att_txz, att_rx.at[j], {"z": zm})
        send(down(0, j), down(2, j), att_txz, att_rx.at[j], {"z": zp})
        return carry

    lax.fori_loop(0, 4, send_own, 0)
    send(att.at[0, core], att.at[0, core], att_txc, att_rxc.at[1], {"c": other})

    def spread():
        for load in loads:
            load.wait()
        lane8 = lax.broadcasted_iota(jnp.int32, (8, 128), 1)
        ints8 = jnp.zeros((8, 128), jnp.int32)
        for i in range(4):
            ints8 = jnp.where(lane8 == i, lens_ref[i], ints8)
            ints8 = jnp.where(lane8 == 4 + i, pairs_ref[0, i], ints8)
            ints8 = jnp.where(lane8 == 8 + i, pairs_ref[1, i], ints8)
            ints8 = jnp.where(lane8 == 12 + i, valid_ref[i], ints8)
        smr[r] = ints8
        vec[0:4, :] = gain_ref[...].astype(F32).reshape(4, 128)
        vec[4:8, :] = head_ref[...].astype(F32).reshape(4, 128)
        vall[t] = vec[...]
        load_r.wait()
        rx[t] = resbuf[pl.ds(pl.multiple_of(t * 16, 16), 16), :]
        acc[...] = jnp.zeros((16, 128), F32)
        hl[...] = jnp.zeros((8, 1024), F32)
        vsum[...] = jnp.zeros((8, 512), F32)

    def pieces(n):
        def one(j, carry):
            tt = wrap(t + j, 16)
            rows = pl.ds(pl.multiple_of(tt * 16, 16), 16)
            send(smr.at[r], smr.at[r], sm_tx, sm_rx, rep_dev(wrap(r + j, 16), t))
            send(vec, vall.at[t], vec_tx, vec_rx, rep_dev(r, tt))
            send(resbuf.at[rows, :], rx.at[t], r1_tx, r1_rx, rep_dev(r, tt))
            return carry

        lax.fori_loop(3 * n - 2, 3 * n + 1, one, 0)

    def gathered():
        await_(vall.at[pl.ds(0, 15)], vec_rx)
        await_(rx.at[pl.ds(0, 15)], r1_rx)
        hgr[...] = vall[:, 0:4, :] * vall[:, 4:8, :]
        for q in range(4):
            hgc[q] = jnp.broadcast_to(hgr[r, q : q + 1, :], (128, 128)).T

    quarters = []
    for q in range(4):
        first = "x" if q < 2 else "y"
        second = "y" if q < 2 else "x"
        a0, b0 = (x, y) if q < 2 else (y, x)
        s = 1 if q % 2 == 0 else -1
        quarters.append(dict(
            q=q, a0=a0, b0=b0, lanes=slice(q * 128, (q + 1) * 128),
            af=wrap(a0 + 2, 4), an=wrap(a0 + s, 4), ao=wrap(a0 - s, 4),
            bf=wrap(b0 + 2, 4), bn=wrap(b0 + s, 4), bo=wrap(b0 - s, 4),
            dan={first: wrap(a0 + s, 4)}, dao={first: wrap(a0 - s, 4)},
            dbn={second: wrap(b0 + s, 4)}, dbo={second: wrap(b0 - s, 4)},
        ))

    def chunk(k, g, a):
        if g["q"] < 2:
            v = pf[k, :, pl.ds(a, 1), :, :, g["lanes"]]
        else:
            v = pf[k, :, :, pl.ds(a, 1), :, g["lanes"]]
        return v.reshape(2, 4, 16, 128)

    def tcol(g, a, b):
        return a * 4 + b if g["q"] < 2 else b * 4 + a

    def ring(n):
        n = jnp.int32(n)
        d, j = n // 4 + 1, lax.rem(n, 4)
        kp, km = 2 * d - 1, 2 * d
        await_(att.at[0, core, pl.ds(0, 128)], att_rx.at[n])

        @pl.when(n < 10)
        def _():
            send(up(kp, j), up(jnp.minimum(kp + 2, 7), j), att_txz, att_rx.at[n + 4], {"z": zm})
            send(down(km, j), down(jnp.minimum(km + 2, 7), j), att_txz, att_rx.at[n + 4], {"z": zp})

        @pl.when((j == 3) & (n < 12))
        def _():
            h = jnp.where((kp == 3) | (kp == 7), 0, 1)
            send(att.at[kp, core], att.at[kp, core], att_txc, att_rxc.at[h], {"c": other})
            h = jnp.where((km == 2) | (km == 6), 0, 1)
            send(att.at[km, core], att.at[km, core], att_txc, att_rxc.at[h], {"c": other})

        @pl.when(n == 13)
        def _():
            send(att.at[7, core], att.at[7, core], att_txc, att_rxc.at[0], {"c": other})

    def step_a(k):
        @pl.when(k > 0)
        def _():
            multiply(k)

        for g in quarters:
            q = g["q"]
            m1s[q, k] = chunk(k, g, g["af"]).astype(BF16)
            send(m1s.at[q, k], m1r.at[q, k], rs_tx.at[0], rs_rx.at[0, k], g["dan"])
        for g in quarters:
            q = g["q"]
            m3s[q, k] = chunk(k, g, g["ao"]).astype(BF16)
            send(m3s.at[q, k], m3r.at[q, k], rs_tx.at[1], rs_rx.at[1, k], g["dao"])

    def step_b(k):
        await_(m1r.at[:, k], rs_rx.at[0, k])
        for g in quarters:
            q = g["q"]
            m2s[q, k] = (chunk(k, g, g["an"]) + m1r[q, k].astype(F32)).astype(BF16)
            send(m2s.at[q, k], m2r.at[q, k], rs_tx.at[2], rs_rx.at[2, k], g["dan"])

    def step_c(k):
        await_(m3r.at[:, k], rs_rx.at[1, k])
        await_(m2r.at[:, k], rs_rx.at[2, k])
        for g in quarters:
            q = g["q"]
            s1f[q, k] = chunk(k, g, g["a0"]) + m2r[q, k].astype(F32) + m3r[q, k].astype(F32)
            n1s[q, k] = s1f[q, k, :, pl.ds(g["bf"], 1)].reshape(2, 16, 128).astype(BF16)
            send(n1s.at[q, k], n1r.at[q, k], rs_tx.at[3], rs_rx.at[3, k], g["dbn"])
            n3s[q, k] = s1f[q, k, :, pl.ds(g["bo"], 1)].reshape(2, 16, 128).astype(BF16)
            send(n3s.at[q, k], n3r.at[q, k], rs_tx.at[4], rs_rx.at[4, k], g["dbo"])

    def step_d(k):
        await_(n1r.at[:, k], rs_rx.at[3, k])
        for g in quarters:
            q = g["q"]
            n2s[q, k] = (s1f[q, k, :, pl.ds(g["bn"], 1)].reshape(2, 16, 128) + n1r[q, k].astype(F32)).astype(BF16)
            send(n2s.at[q, k], n2r.at[q, k], rs_tx.at[5], rs_rx.at[5, k], g["dbn"])

    def step_e(k):
        dz = aim(k)
        sq = jnp.zeros((16, 128), F32)
        await_(n2r.at[:, k], rs_rx.at[5, k])
        await_(n3r.at[:, k], rs_rx.at[4, k])
        for g in quarters:
            q = g["q"]
            total = s1f[q, k, :, pl.ds(g["b0"], 1)].reshape(2, 16, 128) + n2r[q, k].astype(F32) + n3r[q, k].astype(F32)
            total = total + rx[pl.ds(2 * dz, 2), :, g["lanes"]].astype(F32)
            for cc in range(2):
                sq = sq + total[cc] * total[cc]
            high = total.astype(BF16)
            zo[k, :, :, g["lanes"]] = high
            zl[k, :, :, g["lanes"]] = (total - high.astype(F32)).astype(BF16)
        acc[...] += sq
        h = k // 4

        @pl.when(k == 7)
        def _():
            zin[14 + core] = zo[7, core]

        @pl.when(k < 7)
        def _():
            send(zo.at[k, core], zin.at[2 * k + core], zin_tx.at[h], zin_rx.at[h], {"z": dz})

        send(zo.at[k, other], zin.at[2 * k + core], zin_tx.at[h], zin_rx.at[h], {"z": dz, "c": other})

    def halves_of(row):
        high = row.astype(BF16).astype(F32)
        return high, row - high

    def project_head(k):
        for cc in range(2):
            for q in range(4):
                at = slice((cc * 4 + q) * 128, (cc * 4 + q + 1) * 128)
                high, low = halves_of(hgr[2 * aim(k) + cc, q : q + 1, :])
                hl[0:1, at] = high
                hl[1:2, at] = low
        vsum[...] += jnp.dot(hl[...].astype(BF16), wbuf[k], preferred_element_type=F32)

    def head_dots():
        high, rest = halves_of(vsum[0:1, :] + vsum[1:2, :])
        middle, low = halves_of(rest)
        hl[0:1, 0:512] = high
        hl[1:2, 0:512] = middle
        hl[2:3, 0:512] = low
        for q in range(4):
            at = slice(512 + q * 128, 640 + q * 128)
            high, low = halves_of(hgr[t, q : q + 1, :])
            hl[0:1, at] = high
            hl[1:2, at] = low
        rows = hl[...].astype(BF16)
        along = (((1,), (1,)), ((), ()))
        a = lax.dot_general(rows[:, 0:512], att[0, core], along, preferred_element_type=F32)
        b = lax.dot_general(rows[:, 512:1024], resbuf[...], along, preferred_element_type=F32)
        line = a[0:1] + a[1:2] + a[2:3] + b[0:1] + b[1:2]
        dd[t] = jnp.zeros((8, 128), F32)
        dd[t, 0:1, :] = line[:, 0:128]
        dd[t, 1:2, :] = line[:, 128:256]

        def one(j, carry):
            send(dd.at[t], dd.at[t], dd_tx, dd_rx, rep_dev(r, wrap(t + j, 16)))
            return carry

        lax.fori_loop(1, 16, one, 0)

    def send_low(k, carry):
        dz = aim(k)

        @pl.when(k == 7)
        def _():
            zlin[14 + core] = zl[7, core]

        @pl.when(k < 7)
        def _():
            send(zl.at[k, core], zlin.at[2 * k + core], zl_tx, zl_rx, {"z": dz})

        send(zl.at[k, other], zlin.at[2 * k + core], zl_tx, zl_rx, {"z": dz, "c": other})
        return carry

    def flip(h):
        await_(zin.at[pl.ds(0, 8 - h)], zin_rx.at[h])
        v = zin[8 * h : 8 * h + 8].reshape(128, 512).astype(F32)
        for q in range(4):
            za[h, t, q] = v[:, q * 128 : (q + 1) * 128].T.astype(BF16)

    def gsend(h, g, a, b, dev, event):
        q = g["q"]
        tt = tcol(g, g[a], g[b])
        send(za.at[h, tt, q], za.at[h, tt, q], ag_tx, ag_rx.at[h, event], g[dev])

    def gwait(h, event):
        await_(za.at[h, 0], ag_rx.at[h, event])

    def ag1(h):
        for g in quarters:
            gsend(h, g, "a0", "b0", "dan", 0)
            gsend(h, g, "a0", "b0", "dao", 1)

    def ag1cross(h):
        for g in quarters:
            gsend(h, g, "a0", "b0", "dbn", 3)
            gsend(h, g, "a0", "b0", "dbo", 7)

    def ag2(h):
        gwait(h, 0)
        for g in quarters:
            gsend(h, g, "ao", "b0", "dan", 2)
        for g in quarters:
            gsend(h, g, "ao", "b0", "dbn", 4)
        gwait(h, 1)
        for g in quarters:
            gsend(h, g, "an", "b0", "dbn", 5)
        for g in quarters:
            gsend(h, g, "ao", "b0", "dbo", 7)
            gsend(h, g, "an", "b0", "dbo", 7)

    def ag3(h):
        gwait(h, 3)
        for g in quarters:
            gsend(h, g, "a0", "bo", "dbn", 7)
        gwait(h, 2)
        for g in quarters:
            gsend(h, g, "af", "b0", "dbn", 6)
        for g in quarters:
            gsend(h, g, "af", "b0", "dbo", 7)

    def ag4part(h, i):
        gwait(h, 4 + i)
        for g in quarters:
            gsend(h, g, ("ao", "an", "af")[i], "bo", "dbn", 7)

    def ag4(h):
        for i in range(3):
            ag4part(h, i)

    def ag5(h):
        await_(za.at[h, pl.ds(0, 8)], ag_rx.at[h, 7])

    def on(n, parity, first, fn):
        k = (n - first) // 2

        @pl.when((lax.rem(n, 2) == parity) & (n >= first) & (n < first + 16))
        def _():
            fn(k)

    def step(n, carry):
        @pl.when(n == 12)
        def _():
            gathered()

        on(n, 0, 12, step_e)
        on(n, 1, 9, step_d)
        on(n, 0, 6, step_c)
        on(n, 1, 3, step_b)
        on(n, 0, 0, step_a)

        @pl.when(n == 0)
        def _():
            spread()

        @pl.when((n >= 1) & (n < 6))
        def _():
            pieces(n)

        @pl.when((n >= 5) & (lax.rem(n, 2) == 1))
        def _():
            ring((n - 5) // 2)

        @pl.when((n >= 13) & (n < 21))
        def _():
            project_head(n - 13)

        @pl.when(n == 22)
        def _():
            head_dots()

        @pl.when(n == 21)
        def _():
            flip(0)
            ag1(0)

        @pl.when(n == 23)
        def _():
            ag1cross(0)

        return carry

    lax.fori_loop(0, 27, step, 0)

    def absolute(lane):
        slot = lane >> 4
        k = slot >> 1
        m = 7 - (4 * ((k >> 1) & 1) + 2 * (k >> 2) + (k & 1))
        off = ((m + 1) >> 1) * (2 * (m & 1) - 1)
        return ((((zc + off + 8) & 7) * 2 + (slot & 1)) << 4) + (lane & 15)

    rows256 = lax.broadcasted_iota(jnp.int32, (256, 256), 0)
    cols256 = lax.broadcasted_iota(jnp.int32, (256, 256), 1)
    lane16 = lax.broadcasted_iota(jnp.int32, (16, 128), 1)
    row16 = lax.broadcasted_iota(jnp.int32, (16, 128), 0)
    pick = (lane16 & 15) == row16
    sa[r] = jnp.zeros((8, 128), F32)
    ag2(0)
    flip(1)
    ag1(1)
    ag1cross(1)
    column = jnp.sum(acc[...], axis=1, keepdims=True)
    sa[r, 0:1, :] = jnp.sum(jnp.where(pick, column, 0.0), axis=0, keepdims=True)
    await_(dd.at[pl.ds(0, 15)], dd_rx)
    dots = jnp.sum(dd[...], axis=0)
    own_r = lax.broadcasted_iota(jnp.int32, (128, 128), 0)
    own_c = lax.broadcasted_iota(jnp.int32, (128, 128), 1)
    line = jnp.zeros((1, 128), F32)
    for h in range(2):
        own = ((own_r + 128 * h) == (t * 16 + (own_c & 15))).astype(F32)
        line = line + jnp.dot(dots, own, precision=HIGH, preferred_element_type=F32)[h : h + 1, :]
    sa[r, 1:2, :] = line

    def send_sa(j, carry):
        send(sa.at[r], sa.at[r], sa_tx, sa_rx, rep_dev(wrap(r + j, 16), t))
        return carry

    lax.fori_loop(1, 16, send_sa, 0)
    lax.fori_loop(0, 8, send_low, 0)
    ag3(0)
    await_(sa.at[pl.ds(0, 15)], sa_rx)
    sb[t] = jnp.zeros((8, 128), F32)
    for i in range(2):
        for h in range(2):
            line = jnp.zeros((1, 128), F32)
            for j in range(8):
                line = line + jnp.where((lane16[0:1, :] >> 4) == j, sa[8 * h + j, i : i + 1, :], 0.0)
            sb[t, 2 * i + h : 2 * i + h + 1, :] = line

    def send_sb(j, carry):
        send(sb.at[t], sb.at[t], sb_tx, sb_rx, rep_dev(r, wrap(t + j, 16)))
        return carry

    lax.fori_loop(1, 16, send_sb, 0)
    ag2(1)
    ring(11)
    ag4(0)
    ring(12)
    ring(13)
    ag3(1)
    ag4part(1, 0)
    ag4part(1, 1)
    await_(smr.at[pl.ds(0, 15)], sm_rx)
    await_(sb.at[pl.ds(0, 15)], sb_rx)

    ints = smr[:, 0, :].astype(F32)
    tsub = lax.broadcasted_iota(jnp.int32, (16, 128), 0)
    lane = lax.broadcasted_iota(jnp.int32, (16, 128), 1)
    group_r = lax.broadcasted_iota(jnp.int32, (16, 128), 0)
    bl_r = lax.broadcasted_iota(jnp.int32, (128, 128), 0)
    bl_c = lax.broadcasted_iota(jnp.int32, (128, 128), 1)
    block = ((bl_r >> 4) == (bl_c >> 4)).astype(F32)
    eight = lax.broadcasted_iota(jnp.int32, (8, 128), 0)
    halves = []
    count = jnp.zeros((1, 1), F32)
    loss_sum = jnp.zeros((1, 1), F32)
    for h in range(2):
        spread = ((lane >> 4) + 8 * h == group_r).astype(F32)
        ex = lax.dot_general(ints, spread, (((0,), (0,)), ((), ())), precision=HIGH, preferred_element_type=F32)
        lens = [ex[i : i + 1, :] for i in range(4)]
        firsts = [ex[4 + i : 5 + i, :] for i in range(4)]
        seconds = [ex[8 + i : 9 + i, :] for i in range(4)]
        valid = [ex[12 + i : 13 + i, :] for i in range(4)]
        inv = 1.0 / jnp.sqrt(sb[:, h, :] / WIDTH + 1e-05)
        score = inv * sb[:, 2 + h, :]
        lens16 = jnp.zeros((16, 128), F32)
        for i in range(4):
            lens16 = lens16 + jnp.where((tsub >> 2) == i, lens[i], 0.0)
        within = ((tsub & 3) * 16 + (lane & 15)).astype(F32)
        live = (within < lens16).astype(F32)
        pooled = score * live
        stack = jnp.zeros((8, 128), F32)
        for i in range(4):
            part = jnp.sum(jnp.where((tsub >> 2) == i, pooled, 0.0), axis=0, keepdims=True)
            stack = stack + jnp.where(eight == i, part, 0.0)
        summed = jnp.dot(stack, block, precision=HIGH, preferred_element_type=F32)
        reward = [summed[i : i + 1, :] / lens[i] for i in range(4)]
        weights = []
        for p in range(4):
            margin = jnp.zeros((1, 128), F32)
            for i in range(4):
                margin = margin + jnp.where(firsts[p] == i, reward[i], 0.0) - jnp.where(seconds[p] == i, reward[i], 0.0)
            soft = jnp.maximum(-margin, 0.0) + jnp.log1p(jnp.exp(-jnp.abs(margin)))
            loss_sum = loss_sum + jnp.sum(valid[p] * soft, axis=1, keepdims=True) * (1.0 / 16.0)
            count = count + jnp.sum(valid[p], axis=1, keepdims=True) * (1.0 / 16.0)
            weights.append(valid[p] / (1.0 + jnp.exp(margin)))
        halves.append((lens, firsts, seconds, inv, score, live, weights))
    misc_ref[4:8, :] = jnp.broadcast_to(loss_sum / count, (4, 128))
    factor = -scale[0] / count
    for h in range(2):
        lens, firsts, seconds, inv, score, live, weights = halves[h]
        dscore = jnp.zeros((16, 128), F32)
        for i in range(4):
            d = jnp.zeros((1, 128), F32)
            for p in range(4):
                w = weights[p] * factor
                d = d + jnp.where(firsts[p] == i, w, 0.0) - jnp.where(seconds[p] == i, w, 0.0)
            dscore = dscore + jnp.where((tsub >> 2) == i, d / lens[i], 0.0)
        dscore = dscore * live
        ks[:, h * 128 : (h + 1) * 128] = inv * dscore
        cs[:, h * 128 : (h + 1) * 128] = inv * inv * dscore * score * (1.0 / WIDTH)
    to_slot = (rows256 == absolute(cols256)).astype(F32)
    kslot = jnp.dot(ks[...], to_slot, precision=HIGH, preferred_element_type=F32)
    cslot = jnp.dot(cs[...], to_slot, precision=HIGH, preferred_element_type=F32)
    for i in range(16):
        kc[i, 0:1, :] = kslot[i : i + 1, :]
        kc[i, 1:2, :] = cslot[i : i + 1, :]

    await_(zlin.at[pl.ds(0, 15)], zl_rx)
    krow = [kc[t, 0:1, 0:128], kc[t, 0:1, 128:256]]
    gsum = jnp.zeros((8, 128), F32)
    for q in range(4):
        row = jnp.zeros((1, 128), F32)
        for h in range(2):
            column = jnp.broadcast_to(krow[h], (128, 128)).T
            full = zin[8 * h : 8 * h + 8, :, q * 128 : (q + 1) * 128].astype(F32)
            full = full + zlin[8 * h : 8 * h + 8, :, q * 128 : (q + 1) * 128].astype(F32)
            row = row + jnp.sum(full.reshape(128, 128) * column, axis=0, keepdims=True)
        gsum = gsum + jnp.where(eight == q, row, 0.0)
    gmine[...] = gsum

    def send_g(j, carry):
        own = diag & (j == r)

        @pl.when(own)
        def _():
            gr[t] = gmine[...]

        @pl.when(jnp.logical_not(own))
        def _():
            send(gmine, gr.at[t], g_tx, g_rx, rep_dev(j, r))

        return carry

    lax.fori_loop(0, 16, send_g, 0)

    def contract(h, first):
        def group(gi, carry):
            if first:
                @pl.when(gi == 1)
                def _():
                    ag4part(1, 2)

            parts = []
            for j in range(8):
                tt = gi * 8 + j
                k1 = kc[tt, 0:1, h * 128 : (h + 1) * 128]
                c1 = kc[tt, 1:2, h * 128 : (h + 1) * 128]
                for q in range(4):
                    val = hgc[q] * k1 - za[h, tt, q].astype(F32) * c1
                    dt[q * 128 : (q + 1) * 128, j * 128 : (j + 1) * 128] = val.astype(BF16)
                rows = pl.ds(pl.multiple_of(tt * 16, 16), 16)
                for k in range(4 * h, 4 * h + 4):
                    parts.append(att[7 - (4 * (k // 2 % 2) + 2 * (k // 4) + k % 2), :, rows, :].reshape(32, 512))
            rhs = jnp.concatenate(parts, axis=0)
            prod = jnp.dot(dt[...], rhs, preferred_element_type=F32)

            if first:
                @pl.when(gi == 0)
                def _():
                    out_ref[...] = prod

                @pl.when(gi > 0)
                def _():
                    out_ref[...] += prod
            else:
                out_ref[...] += prod
            return carry

        lax.fori_loop(0, 2, group, 0)

    await_(att.at[pl.ds(0, 4), 0], att_rxc.at[0])
    await_(att.at[pl.ds(0, 4), 0], att_rxc.at[1])
    ag5(0)
    contract(0, True)
    ag5(1)
    contract(1, False)

    @pl.when(diag)
    def _():
        await_(gr.at[pl.ds(0, 15)], g_rx)
        await_(gr.at[pl.ds(0, 15)], g_tx)

    @pl.when(jnp.logical_not(diag))
    def _():
        await_(gr, g_rx)
        await_(gr, g_tx)

    misc_ref[0:4, :] = jnp.sum(gr[...], axis=0)[0:4, :]

    await_(rx.at[pl.ds(0, 15)], r1_tx)
    await_(vall.at[pl.ds(0, 15)], vec_tx)
    await_(zin.at[pl.ds(0, 8)], zin_tx.at[0])
    await_(zlin.at[pl.ds(0, 15)], zl_tx)
    await_(zin.at[pl.ds(0, 7)], zin_tx.at[1])
    await_(att.at[pl.ds(0, 7), 0], att_txz)
    await_(att.at[:, 0], att_txc)
    await_(smr.at[pl.ds(0, 15)], sm_tx)
    await_(sa.at[pl.ds(0, 15)], sa_tx)
    await_(dd.at[pl.ds(0, 15)], dd_tx)
    await_(sb.at[pl.ds(0, 15)], sb_tx)
    for i, buf in enumerate((m1s, m3s, m2s, n1s, n3s, n2s)):
        await_(buf, rs_tx.at[i])
    await_(za.at[:, pl.ds(0, 15)], ag_tx)


def shards(attn, out_weight, resid, norm_gain, head, lengths, pairs, pair_valid, loss_scale):
    vm = pltpu.VMEM
    stay = lambda a: pltpu.with_memory_space_constraint(a, pltpu.HBM)
    dma = pltpu.SemaphoreType.DMA
    big = (4, 8, 2, 4, 16, 128)
    little = (4, 8, 2, 16, 128)
    vspec = pl.BlockSpec(memory_space=pltpu.VMEM)
    anyspec = pl.BlockSpec(memory_space=pltpu.HBM)
    smem = pl.BlockSpec(memory_space=pltpu.SMEM)
    out, misc = pl.pallas_call(
        body,
        name="whole",
        out_shape=(jax.ShapeDtypeStruct((512, 512), F32), jax.ShapeDtypeStruct((8, 128), F32)),
        in_specs=[smem] + [anyspec] * 8,
        out_specs=(vspec, vspec),
        scratch_shapes=[
            pltpu.SMEM((4,), jnp.int32), pltpu.SMEM((2, 4), jnp.int32), pltpu.SMEM((4,), jnp.int32),
            vm((512,), BF16), vm((512,), BF16),
            vm((8, 2, 256, 512), BF16), vm((8, 1024, 512), BF16), vm((256, 512), BF16), vm((16, 16, 512), BF16),
            vm((8, 2, 16, 512), BF16), vm((16, 16, 512), BF16), vm((8, 2, 16, 512), BF16), vm((16, 16, 512), BF16), vm((8, 128), F32), vm((16, 8, 128), F32), vm((16, 4, 128), F32),
            vm((16, 128), F32), vm((8, 1024), F32), vm((8, 512), F32), vm((16, 8, 128), F32), vm((16, 8, 128), jnp.int32), vm((8, 2, 4, 4, 16, 512), F32),
            vm(big, BF16), vm(big, BF16), vm(big, BF16), vm(big, BF16), vm(big, BF16), vm(big, BF16), vm(big, F32),
            vm(little, BF16), vm(little, BF16), vm(little, BF16), vm(little, BF16), vm(little, BF16), vm(little, BF16),
            vm((2, 16, 4, 128, 128), BF16), vm((4, 128, 128), F32),
            vm((16, 8, 128), F32), vm((16, 8, 128), F32), vm((16, 256), F32), vm((16, 256), F32), vm((16, 8, 256), F32),
            vm((8, 128), F32), vm((16, 8, 128), F32), vm((512, 1024), BF16),
            dma((2,)), dma((5,)), dma((8,)), dma, dma, dma((14,)), dma((2,)), dma, dma, dma((2,)), dma((2,)), dma, dma, dma, dma, dma, dma,
            dma((6,)), dma((6, 8)), dma, dma((2, 8)), dma, dma, dma, dma, dma, dma, dma, dma,
        ],
        compiler_params=pltpu.CompilerParams(collective_id=0, has_side_effects=True, vmem_limit_bytes=50 * 1024 * 1024),
    )(loss_scale, *(stay(a) for a in (lengths, pairs.T, pair_valid, attn, out_weight, resid, norm_gain, head)))
    g = misc[0:4].reshape(512)
    return (misc[4, 0:1], out, g * head.astype(F32), g * norm_gain.astype(F32))


def solution(mesh):
    finer = Mesh(mesh.devices.reshape(8, 2, 4, 4), ("z", "c", "x", "y"))
    rep, ten = ("z", "c"), ("x", "y")
    placed = (P(rep, ten), P(None, ten), P(rep, ten), P(ten), P(ten), P(rep), P(rep, None), P(rep), P())
    return jax.shard_map(
        shards,
        mesh=finer,
        in_specs=placed,
        out_specs=(P(), P(rep, ten), P(ten), P(ten)),
        check_vma=False,
    )
```
